32 devices in a mesh: beam: 4 (over y, x), row: 4 (over z), col: 2 (over core).
Axes of the slice: x: 2, y: 2, z: 4, core: 2. Of those that a mesh axis runs over, the one named last changes fastest.
Arguments:
- phase_volume: bfloat16 [64, 1024, 256], P('beam', 'row', 'col'), may hold values from -0.75 to 0.75
- absorb_volume: bfloat16 [64, 1024, 256], P('beam', 'row', 'col'), may hold values from -0.375 to 0.375
- probe: float32 [2, 256, 256], replicated, may hold values from -6 to 6
- amplitudes: bfloat16 [4, 2, 32, 256, 256], P('row', 'col', 'beam'), may hold values from 0.19921875 to 2.5
- scan_rows: int32 [4, 2, 32], P('row', 'col', 'beam'), may hold values from 0 to 255
- scan_cols: int32 [4, 2, 32], P('row', 'col', 'beam'), may hold values from 0 to 127
Outputs:
- object_step: float32 [2, 1024, 256], P(None, 'row', 'col')
- probe_gradient: float32 [2, 256, 256], replicated
- loss: float32 [], replicated
The draws below stay inside these ranges and needn't reach their ends.
All inputs are finite; a program needn't handle non-finite values.
Results may differ from the reference program's by a relative error of at most 0.00055.
The reference program's roundings to bfloat16 on the way count: a program that leaves them out, or rounds other values in their place, can miss the bound.
Values sent between devices are 32-bit elements; how exact they have to be, the bound alone decides.
A program may use at most 64 MiB of HBM per device.

```python
import math
import jax
import jax.numpy as jnp
from jax import lax

ROW_DEV = 256
COL_DEV = 128
PROBE = 256
DEPTH = 64
NROWS = 1024
NCOLS = 256
SCANS = 32
N_ROW = 4
N_COL = 2


def touch_ends(result, stream_key, least, largest):
    longest = result.shape.index(max(result.shape))
    spots = []
    for shift in (0, 1):
        where = [jax.random.randint(jax.random.fold_in(stream_key, axis), (), 0, length) for axis, length in enumerate(result.shape)]
        where[longest] = (where[longest] + shift) % result.shape[longest]
        spots.append(tuple(where))
    return result.at[spots[0]].set(least).at[spots[1]].set(largest)


def block_levels(rng, extent, split, least, largest):
    def one(dim, blocks):
        steps = jax.random.uniform(jax.random.fold_in(jax.random.fold_in(rng, 6), dim), (blocks,), jnp.float32, least / len(split), largest / len(split))
        return jnp.repeat(jnp.exp(steps), extent[dim] // blocks).reshape((-1,) + (1,) * (len(extent) - dim - 1))

    loudness = one(*split[0])
    for cut in split[1:]:
        loudness = loudness * one(*cut)
    return loudness


def normal_values(own_key, shape, scale, most, cuts=(), kind=jnp.bfloat16):
    loudness = block_levels(own_key, shape, cuts, -0.22, 0.18) if cuts else 1.0
    values = jax.random.normal(own_key, shape, jnp.float32) * scale * loudness
    return jnp.minimum(jnp.maximum(values, -most), most).astype(kind)


def setup_inputs(seed: int = 0) -> dict:
    seeds = jax.random.split(jax.random.key(seed), 7)
    return {
        "phase_volume": normal_values(seeds[0], (DEPTH, NROWS, NCOLS), DEPTH ** -0.5, 0.75, ((0, 4), (1, 4), (2, 2))),
        "absorb_volume": normal_values(seeds[1], (DEPTH, NROWS, NCOLS), (4 * DEPTH) ** -0.5, 0.375, ((0, 4), (1, 4), (2, 2))),
        "probe": normal_values(seeds[2], (2, PROBE, PROBE), 1.0, 6.0, (), jnp.float32),
        "amplitudes": jnp.clip(0.19921875 + 2.3007812 * jax.random.uniform(seeds[3], (N_ROW, N_COL, SCANS, PROBE, PROBE), jnp.float32) ** block_levels(seeds[3], (N_ROW, N_COL, SCANS, PROBE, PROBE), ((0, 4), (1, 2), (2, 4)), -0.2, 0.2), 0.19921875, 2.5).astype(jnp.bfloat16),
        "scan_rows": touch_ends(jax.random.randint(seeds[4], (N_ROW, N_COL, SCANS), 0, ROW_DEV), jax.random.fold_in(seeds[4], 1), 0, ROW_DEV - 1).astype(jnp.int32),
        "scan_cols": touch_ends(jax.random.randint(seeds[5], (N_ROW, N_COL, SCANS), 0, COL_DEV), jax.random.fold_in(seeds[5], 1), 0, COL_DEV - 1).astype(jnp.int32),
    }


def dft_tables(length):
    indices = jnp.arange(length, dtype=jnp.int32)
    product = indices[:, None] * indices[None, :] % length
    angles = product.astype(jnp.float32) * (2.0 * math.pi / length)
    factor = 1.0 / math.sqrt(length)
    return ((jnp.cos(angles) * factor).astype(jnp.bfloat16), (-jnp.sin(angles) * factor).astype(jnp.bfloat16))

def left_apply(matrix, batch):
    return jnp.einsum('ab,sbc->sac', matrix.astype(jnp.float32), batch.astype(jnp.float32))

def right_apply(batch, matrix):
    return jnp.einsum('sab,bc->sac', batch.astype(jnp.float32), matrix.astype(jnp.float32))

def window_terms(windows, probe, amplitude, table_real, table_imag):
    phase = windows[:, 0]
    absorb = windows[:, 1]
    damping = jnp.exp(-absorb)
    trans_real = damping * jnp.cos(phase)
    trans_imag = damping * jnp.sin(phase)
    wave_real = probe[0] * trans_real - probe[1] * trans_imag
    wave_imag = probe[0] * trans_imag + probe[1] * trans_real
    send_real = wave_real.astype(jnp.bfloat16)
    send_imag = wave_imag.astype(jnp.bfloat16)
    half_real = (left_apply(table_real, send_real) - left_apply(table_imag, send_imag)).astype(jnp.bfloat16)
    half_imag = (left_apply(table_real, send_imag) + left_apply(table_imag, send_real)).astype(jnp.bfloat16)
    far_real = right_apply(half_real, table_real) - right_apply(half_imag, table_imag)
    far_imag = right_apply(half_real, table_imag) + right_apply(half_imag, table_real)
    modulus = jnp.sqrt(far_real * far_real + far_imag * far_imag)
    misfit = jnp.sum((modulus - amplitude) * (modulus - amplitude))
    ratio = 1.0 - amplitude / jnp.maximum(modulus, 0.5)
    resid_real = (far_real * ratio).astype(jnp.bfloat16)
    resid_imag = (far_imag * ratio).astype(jnp.bfloat16)
    back_real = (left_apply(table_real, resid_real) + left_apply(table_imag, resid_imag)).astype(jnp.bfloat16)
    back_imag = (left_apply(table_real, resid_imag) - left_apply(table_imag, resid_real)).astype(jnp.bfloat16)
    grad_real = right_apply(back_real, table_real) + right_apply(back_imag, table_imag)
    grad_imag = right_apply(back_imag, table_real) - right_apply(back_real, table_imag)
    object_real = wave_real * grad_real + wave_imag * grad_imag
    object_imag = wave_real * grad_imag - wave_imag * grad_real
    cells = jnp.stack([object_imag, -object_real], axis=1)
    probe_real = lax.optimization_barrier(jnp.sum(trans_real * grad_real + trans_imag * grad_imag, axis=0))
    probe_imag = lax.optimization_barrier(jnp.sum(trans_real * grad_imag - trans_imag * grad_real, axis=0))
    return (cells, jnp.stack([probe_real, probe_imag]), misfit)

def reference(phase_volume, absorb_volume, probe, amplitudes, scan_rows, scan_cols):
    half = PROBE // 2
    projection = jnp.stack([lax.optimization_barrier(jnp.sum(phase_volume.astype(jnp.float32), axis=0)), lax.optimization_barrier(jnp.sum(absorb_volume.astype(jnp.float32), axis=0))])
    padded = jnp.pad(projection, ((0, 0), (half, half), (half, half)))
    table_real, table_imag = dft_tables(PROBE)
    tiles = N_ROW * N_COL
    row_list = scan_rows.reshape(tiles, SCANS).astype(jnp.int32)
    col_list = scan_cols.reshape(tiles, SCANS).astype(jnp.int32)
    amp_list = amplitudes.reshape(tiles, SCANS, PROBE, PROBE)
    zero_index = jnp.zeros((), jnp.int32)

    def per_tile(carry, inputs):
        canvas, probe_sum, misfit_sum = carry
        tile, rows_here, cols_here, amp_here = inputs
        row_start = (tile // N_COL * ROW_DEV + rows_here).astype(jnp.int32)
        col_start = (tile % N_COL * COL_DEV + cols_here).astype(jnp.int32)
        windows = jax.vmap(lambda row_at, col_at: lax.dynamic_slice(padded, (zero_index, row_at, col_at), (2, PROBE, PROBE)))(row_start, col_start)
        cells, probe_term, misfit = window_terms(windows, probe, amp_here.astype(jnp.float32), table_real, table_imag)

        def add_window(index, canvas_now):
            where = (zero_index, row_start[index], col_start[index])
            piece = lax.dynamic_slice(canvas_now, where, (2, PROBE, PROBE))
            return lax.dynamic_update_slice(canvas_now, piece + cells[index], where)
        canvas = lax.fori_loop(0, SCANS, add_window, canvas)
        return ((canvas, probe_sum + probe_term, misfit_sum + misfit), None)
    start = (jnp.zeros((2, NROWS + PROBE, NCOLS + PROBE), jnp.float32), jnp.zeros((2, PROBE, PROBE), jnp.float32), jnp.zeros((), jnp.float32))
    inputs = (jnp.arange(tiles, dtype=jnp.int32), row_list, col_list, amp_list)
    (canvas, probe_sum, misfit_sum), _ = lax.scan(per_tile, start, inputs)
    gradient = canvas[:, half:half + NROWS, half:half + NCOLS]
    mean_square = jnp.sum(gradient * gradient) / (2 * NROWS * NCOLS)
    factor = jnp.minimum(1.0, 0.5 / jnp.sqrt(mean_square + 1e-06))
    total = N_ROW * N_COL * SCANS
    return (gradient * factor, probe_sum / total, misfit_sum / (total * PROBE * PROBE))
```

```python
import functools
import math

import jax
import jax.numpy as jnp
import numpy as np
from jax import lax
from jax.experimental import pallas as pl
from jax.experimental.pallas import tpu as pltpu
from jax.sharding import PartitionSpec as P


def dft_matrices(length):
    indices = np.arange(length, dtype=np.int32)
    product = indices[:, None] * indices[None, :] % length
    angles = product.astype(np.float32) * np.float32(2.0 * math.pi / length)
    factor = np.float32(1.0 / math.sqrt(length))
    real = (np.cos(angles) * factor).astype(jnp.bfloat16)
    imag = (-np.sin(angles) * factor).astype(jnp.bfloat16)
    left = np.block([[real, -imag], [imag, real]])
    right = np.block([[real, imag], [-imag, real]])
    return jnp.asarray(left), jnp.asarray(right)


def window_kernel(
    rows_ref, cols_ref, trans_ref, probe_ref, amplitude_ref, left_ref, right_ref,
    canvas_ref, term_ref, misfit_ref, kept, wave, half, chi, back,
):
    count, length = amplitude_ref.shape[:2]
    lanes = trans_ref.shape[3]
    blocks = trans_ref.shape[1]
    inner = length // lanes
    step = 32
    steps = length // step
    dot = functools.partial(jnp.dot, preferred_element_type=jnp.float32)
    canvas_ref[...] = jnp.zeros_like(canvas_ref)
    term_ref[...] = jnp.zeros_like(term_ref)
    misfit_ref[...] = jnp.zeros_like(misfit_ref)
    lane = lax.broadcasted_iota(jnp.int32, (step, lanes), 1)

    def enter(w, slot, m):
        row_at, col_at = rows_ref[w], cols_ref[w]
        shift = lax.rem(lanes - col_at, lanes)
        keep = lane < lanes - col_at
        here = pl.ds(m * step, step)
        planes = []
        for part in range(2):
            turned = [
                pltpu.roll(trans_ref[part, k, pl.ds(row_at + m * step, step), :], shift, 1)
                for k in range(blocks)
            ]
            planes.append([jnp.where(keep, turned[k], turned[k + 1]) for k in range(inner)])
        for k in range(inner):
            real, imag = planes[0][k], planes[1][k]
            at = pl.ds(k * lanes, lanes)
            probe_real, probe_imag = probe_ref[0, here, at], probe_ref[1, here, at]
            kept[slot, 0, here, at] = real
            kept[slot, 1, here, at] = imag
            wave[slot, pl.ds(m * step, step), at] = (probe_real * real - probe_imag * imag).astype(jnp.bfloat16)
            wave[slot, pl.ds(length + m * step, step), at] = (probe_real * imag + probe_imag * real).astype(jnp.bfloat16)

    def compare(w, slot, m, far):
        rows = far.shape[0]
        here = pl.ds(m, rows)
        real, imag = far[:, :length], far[:, length:]
        amplitude = amplitude_ref[w, here, :].astype(jnp.float32)
        square = real * real + imag * imag
        inverse = lax.rsqrt(jnp.maximum(square, 1.2e-38))
        off = square * inverse - amplitude
        misfit_ref[...] += jnp.sum((off * off).reshape(rows // 8, 8, length), axis=0)
        ratio = 1.0 - amplitude * jnp.minimum(inverse, 2.0)
        chi[slot, here, :] = (real * ratio).astype(jnp.bfloat16)
        chi[slot, pl.ds(length + m, rows), :] = (imag * ratio).astype(jnp.bfloat16)

    def leave(w, slot, m, grad):
        rows = grad.shape[0]
        row_at, col_at = rows_ref[w], cols_ref[w]
        here = pl.ds(m, rows)
        lane = lax.broadcasted_iota(jnp.int32, (rows, lanes), 1)
        first = lane >= col_at
        objects = [[], []]
        for k in range(inner):
            at = pl.ds(k * lanes, lanes)
            grad_real = grad[:, k * lanes : (k + 1) * lanes]
            grad_imag = grad[:, length + k * lanes : length + (k + 1) * lanes]
            real, imag = kept[slot, 0, here, at], kept[slot, 1, here, at]
            term_real = real * grad_real + imag * grad_imag
            term_imag = real * grad_imag - imag * grad_real
            term_ref[0, here, at] += term_real
            term_ref[1, here, at] += term_imag
            probe_real, probe_imag = probe_ref[0, here, at], probe_ref[1, here, at]
            objects[0].append(pltpu.roll(probe_real * term_imag - probe_imag * term_real, col_at, 1))
            objects[1].append(pltpu.roll(probe_real * term_real + probe_imag * term_imag, col_at, 1))
        there = pl.ds(row_at + m, rows)
        for part in range(2):
            turned = objects[part]
            for k in range(blocks):
                before = turned[k - 1] if k > 0 else 0.0
                after = turned[k] if k < inner else 0.0
                value = jnp.where(first, after, before)
                if part:
                    canvas_ref[part, k, there, :] -= value
                else:
                    canvas_ref[part, k, there, :] += value

    def left(values, first, out, slot):
        part = dot(first[...], values[slot])
        out[slot, :, :length] = part[:length].astype(jnp.bfloat16)
        out[slot, :, length:] = part[length:].astype(jnp.bfloat16)

    def far_of(w, slot):
        far = dot(half[slot], right_ref[...])
        return [functools.partial(compare, w, slot, m * step, far[m * step : (m + 1) * step]) for m in range(steps)]

    def near_of(w, slot):
        near = dot(back[slot], left_ref[...])
        return [functools.partial(leave, w, slot, m * step, near[m * step : (m + 1) * step]) for m in range(steps)]

    def run(parts):
        for part in parts:
            part()

    def enters(w):
        return [functools.partial(enter, w, w % 2, m) for m in range(steps)] if w < count else []

    def halves(make, source, table, w, slot, cut):
        tall = length // cut
        for c in range(cut):
            out = dot(source[slot, c * tall : (c + 1) * tall], table[...])
            for m in range(tall // step):
                make(w, slot, c * tall + m * step, out[m * step : (m + 1) * step])

    run(enters(0))
    for p in range(count // 2):
        a, b = 2 * p, 2 * p + 1
        left(wave, left_ref, half, 0)
        if p:
            halves(leave, back, left_ref, b - 2, 1, 2)
        run(enters(b))
        left(wave, left_ref, half, 1)
        halves(compare, half, right_ref, a, 0, 2)
        left(chi, right_ref, back, 0)
        halves(compare, half, right_ref, b, 1, 2)
        left(chi, right_ref, back, 1)
        halves(leave, back, left_ref, a, 0, 2)
        run(enters(a + 2))
    halves(leave, back, left_ref, count - 1, 1, 2)


def window_terms(trans, probe, amplitude, rows, cols):
    count, length = amplitude.shape[:2]
    left, right = dft_matrices(length)
    f32, bf16 = jnp.float32, jnp.bfloat16
    smem = pl.BlockSpec(memory_space=pltpu.SMEM)
    return pl.pallas_call(
        window_kernel,
        out_shape=[
            jax.ShapeDtypeStruct(trans.shape, f32),
            jax.ShapeDtypeStruct(probe.shape, f32),
            jax.ShapeDtypeStruct((8, length), f32),
        ],
        in_specs=[smem, smem] + vmem_specs(5),
        out_specs=vmem_specs(3),
        scratch_shapes=[
            pltpu.VMEM((2, 2, length, length), f32),
            pltpu.VMEM((2, 2 * length, length), bf16),
            pltpu.VMEM((2, length, 2 * length), bf16),
            pltpu.VMEM((2, 2 * length, length), bf16),
            pltpu.VMEM((2, length, 2 * length), bf16),
        ],
        compiler_params=pltpu.CompilerParams(vmem_limit_bytes=40 * 2**20),
    )(rows, cols, trans, probe, amplitude, left, right)


def partners(me, count):
    if count % 4 == 0:
        high, low = me // 4 * 4 + me % 4 // 2 * 2, me % 2
        flips = [(1, 1), (0, 1), (1, 0)]
        near = []
        for up, across in flips:
            other = me // 4 * 4 + lax.rem(me % 4 // 2 + up, 2) * 2 + lax.rem(low + across, 2)
            near.append(other)
        if count == 4:
            return near
    return [lax.rem(me + d, count) for d in range(1, count)]


class Sends:
    def __init__(self, sizes, send_sem, recv_sem):
        self.axes = {axis: (lax.axis_index(axis), count) for axis, count in sizes}
        self.sends, self.recvs, self.used = send_sem, recv_sem, 0
        self.started = []

    def greet(self, groups):
        barrier = pltpu.get_barrier_semaphore()
        for target in groups:
            pl.semaphore_signal(barrier, inc=1, device_id=target, device_id_type=pl.DeviceIdType.MESH)
        pl.semaphore_wait(barrier, len(groups))

    def others(self, axis):
        return partners(*self.axes[axis])

    def copy(self, target, src, dst):
        index = self.used
        self.used += 1
        return pltpu.make_async_remote_copy(
            src_ref=src, dst_ref=dst, send_sem=self.sends.at[index],
            recv_sem=self.recvs.at[index], device_id=target,
            device_id_type=pl.DeviceIdType.MESH,
        )

    def send(self, target, src, dst):
        one = self.copy(target, src, dst)
        one.start()
        self.started.append(one.wait_send)
        return one

    def sides(self, axis, down, up, to_before=True, to_after=True):
        me, count = self.axes[axis]
        both = jnp.logical_and
        sends_before, sends_after = both(me > 0, to_before), both(me < count - 1, to_after)
        gets_after, gets_before = both(me < count - 1, to_before), both(me > 0, to_after)
        before = self.copy({axis: lax.rem(me + count - 1, count)}, *down)
        after = self.copy({axis: lax.rem(me + 1, count)}, *up)
        pl.when(sends_before)(before.start)
        pl.when(sends_after)(after.start)

        def wait_send():
            pl.when(sends_before)(before.wait_send)
            pl.when(sends_after)(after.wait_send)

        def wait_recv():
            pl.when(gets_after)(before.wait_recv)
            pl.when(gets_before)(after.wait_recv)

        self.started.append(wait_send)
        return wait_recv

    def finish(self):
        for wait_send in self.started:
            wait_send()


def project_kernel(sizes, half, phase_ref, absorb_ref, out_ref, volume, part, slots, load_sem, send_sem, recv_sem):
    net = Sends(sizes, send_sem, recv_sem)
    beam, beams = net.axes["beam"]
    depth, rows, cols = phase_ref.shape
    share = rows // beams
    edge = half // share
    blocks = out_ref.shape[2]
    peers = net.others("beam")
    order = peers + [beam]
    loads = []
    for i, peer in enumerate(order):
        here = pl.ds(pl.multiple_of(peer * share, share), share)
        for plane, ref in enumerate((phase_ref, absorb_ref)):
            one = pltpu.make_async_copy(ref.at[:, here, :], volume.at[plane, i], load_sem.at[plane, i])
            one.start()
            loads.append(one)
    out_ref[0] = jnp.ones(out_ref.shape[1:], jnp.float32)
    out_ref[1] = jnp.zeros(out_ref.shape[1:], jnp.float32)
    targets = [{axis: peer} for axis in net.axes for peer in net.others(axis)]
    net.greet(targets)
    scatter = []
    for i, peer in enumerate(order):
        for plane in range(2):
            loads[2 * i + plane].wait()
            total = volume[plane, i, 0].astype(jnp.float32)
            for d in range(1, depth):
                total += volume[plane, i, d].astype(jnp.float32)
            part[i, plane] = total
        if i < beams - 1:
            scatter.append(net.send({"beam": peer}, part.at[i], slots.at[i]))
    total = part[beams - 1]
    for i, one in enumerate(scatter):
        one.wait_recv()
        total += slots[i]
    damping = jnp.exp(-total[1])
    own = edge + beam
    out_ref[0, 1, own] = damping * jnp.cos(total[0])
    out_ref[1, 1, own] = damping * jnp.sin(total[0])
    at = lambda side, block: out_ref.at[:, side, block]
    arrivals = []

    def across(block, when=True):
        arrivals.append(net.sides("col", (at(1, block), at(2, block)), (at(1, block), at(0, block)), when, when))

    def along(share_at):
        here = at(1, edge + share_at)
        below = lax.rem(edge + beams + share_at, blocks)
        above = lax.rem(edge + share_at + blocks - beams, blocks)
        wait = net.sides(
            "row", (here, at(1, below)), (here, at(1, above)), share_at < edge, share_at >= beams - edge
        )
        return wait, share_at, below, above

    row, rows_count = net.axes["row"]
    gather = [net.send({"beam": peer}, at(1, own), at(1, own)) for peer in peers]
    rims = [along(beam)]
    across(own)
    for peer, one in zip(peers, gather):
        one.wait_recv()
        rims.append(along(peer))
        across(edge + peer)
    for wait, share_at, below, above in rims:
        wait()
        across(below, jnp.logical_and(row < rows_count - 1, share_at < edge))
        across(above, jnp.logical_and(row > 0, share_at >= beams - edge))
    for wait in arrivals:
        wait()
    net.finish()


def comm_params(number):
    return pltpu.CompilerParams(
        collective_id=number, has_side_effects=True, vmem_limit_bytes=40 * 2**20
    )


def vmem_specs(count):
    return [pl.BlockSpec(memory_space=pltpu.VMEM)] * count


def project(sizes, half, phase_volume, absorb_volume):
    depth, rows, cols = phase_volume.shape
    assert half == cols
    beams = dict(sizes)["beam"]
    share = rows // beams
    f32 = jnp.float32
    tall = rows + 2 * half
    wires = 2 * beams + 2 * beams + 6 * beams
    trans = pl.pallas_call(
        functools.partial(project_kernel, sizes, half),
        out_shape=jax.ShapeDtypeStruct((2, 3, tall // share, share, cols), f32),
        in_specs=[pl.BlockSpec(memory_space=pltpu.HBM)] * 2,
        out_specs=vmem_specs(1)[0],
        scratch_shapes=[
            pltpu.VMEM((2, beams, depth, share, cols), phase_volume.dtype),
            pltpu.VMEM((beams, 2, share, cols), f32),
            pltpu.VMEM((beams - 1, 2, share, cols), f32),
            pltpu.SemaphoreType.DMA((2, beams)),
            pltpu.SemaphoreType.DMA((wires,)),
            pltpu.SemaphoreType.DMA((wires,)),
        ],
        compiler_params=comm_params(1),
    )(phase_volume, absorb_volume)
    return trans.reshape(2, 3, tall, cols)


def combine_kernel(
    sizes, half, entries, positions, canvas_ref, term_ref, misfit_ref,
    grad_ref, probe_ref, scalar_ref,
    side, strip, rims, folded, folded_in,
    term_col, term_a, term_beam, term_b, term_row, small, small_col,
    send_sem, recv_sem,
):
    net = Sends(sizes, send_sem, recv_sem)
    beam, beams = net.axes["beam"]
    row, rows_count = net.axes["row"]
    col, cols_count = net.axes["col"]
    blocks = strip.shape[1]
    cols = strip.shape[4]
    beam_peers, row_peers, col_peers = (net.others(axis) for axis in ("beam", "row", "col"))
    order = beam_peers + [beam]
    row_order = row_peers + [row]
    wide = [{"beam": b, "row": r} for b in order for r in row_order][:-1]
    rims[...] = jnp.zeros_like(rims)

    @pl.when(col == 0)
    def _():
        side[0] = jnp.zeros(side.shape[1:], jnp.float32)

    @pl.when(col == cols_count - 1)
    def _():
        side[1] = jnp.zeros(side.shape[1:], jnp.float32)

    net.greet(wide + [{"col": c} for c in col_peers])

    across, term_across = [], []
    for p in order:
        term_across.append([
            net.send({"col": c}, term_ref.at[c, p], term_col.at[k, p]) for k, c in enumerate(col_peers)
        ])
        across.append(net.sides(
            "col",
            (canvas_ref.at[:, 0, :, p], side.at[1, :, :, p]),
            (canvas_ref.at[:, 2, :, p], side.at[0, :, :, p]),
        ))
    along, term_beams = [], []
    for i, p in enumerate(order):
        for one in term_across[i]:
            one.wait_recv()
        total = term_ref[col, p]
        for k in range(cols_count - 1):
            total += term_col[k, p]
        term_a[i] = total
        if i < beams - 1:
            term_beams.append([
                net.send({"beam": p}, term_a.at[i, r], term_beam.at[i, r]) for r in row_order
            ])
        across[i]()
        strip[:, :, p] = canvas_ref[:, 1, :, p] + side[0, :, :, p] + side[1, :, :, p]
        along.append(net.sides(
            "row",
            (strip.at[:, 0, p], rims.at[1, :, p]),
            (strip.at[:, blocks - 1, p], rims.at[0, :, p]),
        ))

    grids = []
    for i, p in enumerate(order):
        along[i]()
        middle = strip[:, 1 : blocks - 1, p]
        folded[i] = middle
        folded[i, :, 0] += rims[0, :, p]
        folded[i, :, blocks - 3] += rims[1, :, p]
        if i < beams - 1:
            grids.append(net.send({"beam": p}, folded.at[i], folded_in.at[i]))
    term_rows = []
    for k, r in enumerate(row_order):
        total = term_a[beams - 1, r]
        for i in range(beams - 1):
            term_beams[i][k].wait_recv()
            total += term_beam[i, r]
        term_b[k] = total
        if k < rows_count - 1:
            term_rows.append(net.send({"row": r}, term_b.at[k], term_row.at[k]))

    total = folded[beams - 1]
    for i, one in enumerate(grids):
        one.wait_recv()
        total += folded_in[i]
    grad_ref[:, :, beam] = total
    misfit_sum = misfit_ref[:, :cols]
    for k in range(1, misfit_ref.shape[1] // cols):
        misfit_sum += misfit_ref[:, k * cols : (k + 1) * cols]
    small[beam, row, 0] = jnp.sum((total * total).reshape(-1, 8, cols), axis=0)
    small[beam, row, 1] = misfit_sum
    smalls = [net.send(target, small.at[beam, row], small.at[beam, row]) for target in wide]
    mine = grad_ref.at[:, :, beam]
    grads = [net.send({"beam": p}, mine, mine) for p in beam_peers]

    total = term_b[rows_count - 1]
    for k, one in enumerate(term_rows):
        one.wait_recv()
        total += term_row[k]
    probe_ref[col, beam, row] = total * (1.0 / positions)
    piece = lambda b, r: probe_ref.at[col, b, r]
    row_copies = [net.send({"row": r}, piece(beam, row), piece(beam, row)) for r in row_peers]
    beam_copies = [[net.send({"beam": p}, piece(beam, row), piece(beam, row)) for p in beam_peers]]
    for one, r in zip(row_copies, row_peers):
        one.wait_recv()
        beam_copies.append([net.send({"beam": p}, piece(beam, r), piece(beam, r)) for p in beam_peers])
    col_copies = [net.send({"col": c}, probe_ref.at[col, beam], probe_ref.at[col, beam]) for c in col_peers]

    for one in smalls:
        one.wait_recv()
    total = small[0, 0]
    for k in range(1, beams * rows_count):
        total += small[k // rows_count, k % rows_count]
    small_col[col] = total
    small_copies = [net.send({"col": c}, small_col.at[col], small_col.at[col]) for c in col_peers]

    for i, p in enumerate(beam_peers):
        for group in beam_copies:
            group[i].wait_recv()
        col_copies += [net.send({"col": c}, probe_ref.at[col, p], probe_ref.at[col, p]) for c in col_peers]
    for one in small_copies:
        one.wait_recv()
    total = small_col[0]
    for k in range(1, cols_count):
        total += small_col[k]
    mean_square = jnp.sum(total[0], keepdims=True) / entries
    factor = jnp.minimum(1.0, 0.5 / jnp.sqrt(mean_square + 1e-06))
    scalar_ref[0] = jnp.broadcast_to(factor, scalar_ref.shape[1:])
    scalar_ref[1] = jnp.broadcast_to(jnp.sum(total[1], keepdims=True), scalar_ref.shape[1:])
    for one in grads + col_copies:
        one.wait_recv()
    net.finish()


def close_kernel(scale, grad_ref, probe_ref, scalar_ref, step_ref, gradient_ref, loss_ref, step, loss, sems):
    first = pltpu.make_async_copy(probe_ref, gradient_ref, sems.at[0])
    first.start()
    factor = scalar_ref[0, :1, :1]
    step[...] = grad_ref[...] * factor[None, None, None]
    second = pltpu.make_async_copy(step, step_ref, sems.at[1])
    second.start()
    loss[...] = scalar_ref[1, :1, :1] * scale
    third = pltpu.make_async_copy(loss, loss_ref, sems.at[2])
    third.start()
    first.wait()
    second.wait()
    third.wait()


def combine(sizes, half, rows, cols, positions, canvas, term, misfit):
    counts = dict(sizes)
    beams, rows_count, cols_count = counts["beam"], counts["row"], counts["col"]
    f32 = jnp.float32
    blocks = rows // half + 2
    thin = half // beams
    lines = term.shape[0] * term.shape[1] // (cols_count * beams * rows_count)
    width = term.shape[2]
    pieces = (cols_count, beams, rows_count, lines, width)
    entries = 2 * rows * cols * rows_count * cols_count
    wires = (
        (cols_count - 1) * 2 * beams + 5 * beams + (beams - 1) * 2 * rows_count
        + 2 * (rows_count - 1) + 2 * (beams - 1) + beams * rows_count + cols_count
    )
    grid = (2, blocks - 2, beams, thin, cols)
    shape = jax.ShapeDtypeStruct
    grad, probe_gradient, scalars = pl.pallas_call(
        functools.partial(combine_kernel, sizes, half, entries, positions),
        out_shape=[shape(grid, f32), shape(pieces, f32), shape((2, 8, 128), f32)],
        in_specs=vmem_specs(3),
        out_specs=vmem_specs(3),
        scratch_shapes=[
            pltpu.VMEM((2, 2, blocks, beams, thin, cols), f32),
            pltpu.VMEM((2, blocks, beams, thin, cols), f32),
            pltpu.VMEM((2, 2, beams, thin, cols), f32),
            pltpu.VMEM((beams, 2, blocks - 2, thin, cols), f32),
            pltpu.VMEM((beams - 1, 2, blocks - 2, thin, cols), f32),
            pltpu.VMEM((cols_count - 1,) + pieces[1:], f32),
            pltpu.VMEM(pieces[1:], f32),
            pltpu.VMEM((beams - 1,) + pieces[2:], f32),
            pltpu.VMEM(pieces[2:], f32),
            pltpu.VMEM((rows_count - 1,) + pieces[3:], f32),
            pltpu.VMEM((beams, rows_count, 2, 8, cols), f32),
            pltpu.VMEM((cols_count, 2, 8, cols), f32),
            pltpu.SemaphoreType.DMA((wires,)),
            pltpu.SemaphoreType.DMA((wires,)),
        ],
        compiler_params=comm_params(2),
    )(canvas.reshape(2, 3, blocks, beams, thin, cols), term.reshape(pieces), misfit)
    probe_gradient = probe_gradient.reshape(term.shape)
    anywhere = pl.BlockSpec(memory_space=pltpu.HBM)
    step, probe_gradient, loss = pl.pallas_call(
        functools.partial(close_kernel, 1.0 / (positions * width * width)),
        out_shape=[shape(grid, f32), shape(term.shape, f32), shape((1, 1), f32)],
        in_specs=vmem_specs(3),
        out_specs=[anywhere] * 3,
        scratch_shapes=[
            pltpu.VMEM(grid, f32), pltpu.VMEM((1, 1), f32), pltpu.SemaphoreType.DMA((3,)),
        ],
    )(grad, probe_gradient, scalars)
    return step.reshape(2, rows, cols), probe_gradient, loss.reshape(())


def local(phase_volume, absorb_volume, probe, amplitudes, scan_rows, scan_cols):
    length = probe.shape[1]
    half = length // 2
    count = scan_rows.shape[2]
    rows, cols = phase_volume.shape[1:]
    sizes = tuple((axis, lax.axis_size(axis)) for axis in ("beam", "row", "col"))
    trans = project(sizes, half, phase_volume, absorb_volume)
    canvas, term, misfit = window_terms(
        trans, probe, amplitudes.reshape(count, length, length),
        scan_rows.reshape(count), scan_cols.reshape(count),
    )
    positions = count * math.prod(size for _, size in sizes)
    return combine(sizes, half, rows, cols, positions, canvas, term, misfit)


def solution(mesh):
    in_specs = (
        P("beam", "row", "col"),
        P("beam", "row", "col"),
        P(),
        P("row", "col", "beam", None, None),
        P("row", "col", "beam"),
        P("row", "col", "beam"),
    )
    out_specs = (P(None, "row", "col"), P(), P())
    return jax.shard_map(local, mesh=mesh, in_specs=in_specs, out_specs=out_specs, check_vma=False)
```

```python
import functools
import math

import jax
import jax.numpy as jnp
import numpy as np
from jax import lax
from jax.experimental import pallas as pl
from jax.experimental.pallas import tpu as pltpu
from jax.sharding import PartitionSpec as P


def dft_matrices(length):
    indices = np.arange(length, dtype=np.int32)
    product = indices[:, None] * indices[None, :] % length
    angles = product.astype(np.float32) * np.float32(2.0 * math.pi / length)
    factor = np.float32(1.0 / math.sqrt(length))
    real = (np.cos(angles) * factor).astype(jnp.bfloat16)
    imag = (-np.sin(angles) * factor).astype(jnp.bfloat16)
    left = np.block([[real, -imag], [imag, real]])
    right = np.block([[real, imag], [-imag, real]])
    return jnp.asarray(left), jnp.asarray(right)


def partners(me, count):
    if count % 4 == 0:
        high, low = me // 4 * 4 + me % 4 // 2 * 2, me % 2
        flips = [(1, 1), (0, 1), (1, 0)]
        near = []
        for up, across in flips:
            other = me // 4 * 4 + lax.rem(me % 4 // 2 + up, 2) * 2 + lax.rem(low + across, 2)
            near.append(other)
        if count == 4:
            return near
    return [lax.rem(me + d, count) for d in range(1, count)]


class Sends:
    def __init__(self, sizes, send_sem, recv_sem):
        self.axes = {axis: (lax.axis_index(axis), count) for axis, count in sizes}
        self.sends, self.recvs, self.used = send_sem, recv_sem, 0
        self.started = []

    def greet(self, groups):
        barrier = pltpu.get_barrier_semaphore()
        for target in groups:
            pl.semaphore_signal(barrier, inc=1, device_id=target, device_id_type=pl.DeviceIdType.MESH)
        pl.semaphore_wait(barrier, len(groups))

    def others(self, axis):
        return partners(*self.axes[axis])

    def copy(self, target, src, dst):
        index = self.used
        self.used += 1
        return pltpu.make_async_remote_copy(
            src_ref=src, dst_ref=dst, send_sem=self.sends.at[index],
            recv_sem=self.recvs.at[index], device_id=target,
            device_id_type=pl.DeviceIdType.MESH,
        )

    def send(self, target, src, dst):
        one = self.copy(target, src, dst)
        one.start()
        self.started.append(one.wait_send)
        return one

    def sides(self, axis, down, up, to_before=True, to_after=True):
        me, count = self.axes[axis]
        both = jnp.logical_and
        sends_before, sends_after = both(me > 0, to_before), both(me < count - 1, to_after)
        gets_after, gets_before = both(me < count - 1, to_before), both(me > 0, to_after)
        before = self.copy({axis: lax.rem(me + count - 1, count)}, *down)
        after = self.copy({axis: lax.rem(me + 1, count)}, *up)
        pl.when(sends_before)(before.start)
        pl.when(sends_after)(after.start)

        def wait_send():
            pl.when(sends_before)(before.wait_send)
            pl.when(sends_after)(after.wait_send)

        def wait_recv():
            pl.when(gets_after)(before.wait_recv)
            pl.when(gets_before)(after.wait_recv)

        self.started.append(wait_send)
        return wait_recv

    def finish(self):
        for wait_send in self.started:
            wait_send()


def vmem_specs(count):
    return [pl.BlockSpec(memory_space=pltpu.VMEM)] * count


def project(net, half, phase_ref, absorb_ref, out_ref, volume, part, slots, load_sem):
    beam, beams = net.axes["beam"]
    row, rows_count = net.axes["row"]
    depth, rows, cols = phase_ref.shape
    share = rows // beams
    edge = half // share
    blocks = rows // share + 2 * edge
    peers = net.others("beam")
    order = peers + [beam]
    loads = []
    for i, peer in enumerate(order):
        here = pl.ds(pl.multiple_of(peer * share, share), share)
        for plane, ref in enumerate((phase_ref, absorb_ref)):
            one = pltpu.make_async_copy(ref.at[:, here, :], volume.at[plane, i], load_sem.at[plane, i])
            one.start()
            loads.append(one)
    yield
    scatter = []
    for i, peer in enumerate(order):
        for plane in range(2):
            loads[2 * i + plane].wait()
            total = volume[plane, i, 0].astype(jnp.float32)
            for d in range(1, depth):
                total += volume[plane, i, d].astype(jnp.float32)
            part[i, plane] = total
        if i == 0:
            net.greet([{axis: other} for axis in net.axes for other in net.others(axis)])
        if i < beams - 1:
            scatter.append(net.send({"beam": peer}, part.at[i], slots.at[i]))
    total = part[beams - 1]
    for i, one in enumerate(scatter):
        one.wait_recv()
        total += slots[i]
    at = lambda side, block: out_ref.at[:, side, pl.ds(pl.multiple_of(block * share, share), share), :]
    damping = jnp.exp(-total[1])
    own = edge + beam
    here = pl.ds(pl.multiple_of(own * share, share), share)
    out_ref[0, 1, here, :] = damping * jnp.cos(total[0])
    out_ref[1, 1, here, :] = damping * jnp.sin(total[0])
    arrivals = []

    def across(block, when=True):
        arrivals.append(net.sides("col", (at(1, block), at(2, block)), (at(1, block), at(0, block)), when, when))

    def along(share_at):
        here = at(1, edge + share_at)
        below = lax.rem(edge + beams + share_at, blocks)
        above = lax.rem(edge + share_at + blocks - beams, blocks)
        wait = net.sides(
            "row", (here, at(1, below)), (here, at(1, above)), share_at < edge, share_at >= beams - edge
        )
        return wait, share_at, below, above

    gather = [net.send({"beam": peer}, at(1, own), at(1, own)) for peer in peers]
    rims = [along(beam)]
    across(own)
    for peer, one in zip(peers, gather):
        one.wait_recv()
        rims.append(along(peer))
        across(edge + peer)
    for wait, share_at, below, above in rims:
        wait()
        across(below, jnp.logical_and(row < rows_count - 1, share_at < edge))
        across(above, jnp.logical_and(row > 0, share_at >= beams - edge))
    for wait in arrivals:
        wait()
    yield


def windows(
    rows_ref, cols_ref, trans_ref, probe_ref, amplitude_ref, left_ref, right_ref,
    canvas_ref, term_ref, misfit_ref, kept, wave, half, chi, back, moved,
):
    count, length = amplitude_ref.shape[:2]
    lanes = trans_ref.shape[3]
    spans = trans_ref.shape[1]
    inner = length // lanes
    step = 32
    steps = length // step
    dot = functools.partial(jnp.dot, preferred_element_type=jnp.float32)
    lane = lax.broadcasted_iota(jnp.int32, (step, lanes), 1)
    places = moved.shape[0]

    def enter(w, slot, m):
        row_at, col_at = rows_ref[w], cols_ref[w]
        shift = lax.rem(lanes - col_at, lanes)
        keep = lane < lanes - col_at
        here = pl.ds(m * step, step)
        planes = []
        for part in range(2):
            turned = [
                pltpu.roll(trans_ref[part, k, pl.ds(row_at + m * step, step), :], shift, 1)
                for k in range(spans)
            ]
            planes.append([jnp.where(keep, turned[k], turned[k + 1]) for k in range(inner)])
        for k in range(inner):
            real, imag = planes[0][k], planes[1][k]
            at = pl.ds(k * lanes, lanes)
            probe_real, probe_imag = probe_ref[0, here, at], probe_ref[1, here, at]
            kept[slot, 0, here, at] = real
            kept[slot, 1, here, at] = imag
            wave[slot, pl.ds(m * step, step), at] = (probe_real * real - probe_imag * imag).astype(jnp.bfloat16)
            wave[slot, pl.ds(length + m * step, step), at] = (probe_real * imag + probe_imag * real).astype(jnp.bfloat16)

    def compare(w, slot, m, far):
        here = pl.ds(m, step)
        real, imag = far[:, :length], far[:, length:]
        amplitude = amplitude_ref[w, here, :].astype(jnp.float32)
        square = real * real + imag * imag
        inverse = lax.rsqrt(jnp.maximum(square, 1.2e-38))
        off = square * inverse - amplitude
        misfit_ref[...] += jnp.sum((off * off).reshape(step // 8, 8, length), axis=0)
        ratio = 1.0 - amplitude * jnp.minimum(inverse, 2.0)
        chi[slot, here, :] = (real * ratio).astype(jnp.bfloat16)
        chi[slot, pl.ds(length + m, step), :] = (imag * ratio).astype(jnp.bfloat16)

    def leave(w, slot, m, grad):
        col_at = cols_ref[w]
        here = pl.ds(m, step)
        first = lane >= col_at
        objects = [[], []]
        for k in range(inner):
            at = pl.ds(k * lanes, lanes)
            grad_real = grad[:, k * lanes : (k + 1) * lanes]
            grad_imag = grad[:, length + k * lanes : length + (k + 1) * lanes]
            real, imag = kept[slot, 0, here, at], kept[slot, 1, here, at]
            term_real = real * grad_real + imag * grad_imag
            term_imag = real * grad_imag - imag * grad_real
            if w == 0:
                term_ref[0, here, at] = term_real
                term_ref[1, here, at] = term_imag
            else:
                term_ref[0, here, at] += term_real
                term_ref[1, here, at] += term_imag
            probe_real, probe_imag = probe_ref[0, here, at], probe_ref[1, here, at]
            objects[0].append(pltpu.roll(probe_real * term_imag - probe_imag * term_real, col_at, 1))
            objects[1].append(pltpu.roll(probe_real * term_real + probe_imag * term_imag, col_at, 1))
        for part in range(2):
            turned = objects[part]
            for k in range(spans):
                before = turned[k - 1] if k > 0 else 0.0
                after = turned[k] if k < inner else 0.0
                moved[w % places, part, k, pl.ds(length + m, step), :] = jnp.where(first, after, before)

    def left(values, first, out, slot):
        part = dot(first[...], values[slot])
        out[slot, :, :length] = part[:length].astype(jnp.bfloat16)
        out[slot, :, length:] = part[length:].astype(jnp.bfloat16)

    def halves(make, source, table, w, slot, cut):
        tall = length // cut
        for c in range(cut):
            out = dot(source[slot, c * tall : (c + 1) * tall], table[...])
            for m in range(tall // step):
                make(w, slot, c * tall + m * step, out[m * step : (m + 1) * step])

    def enters(w):
        if w < count:
            for m in range(steps):
                enter(w, w % 2, m)

    def place(pair, block, b, k):
        thin = canvas_ref.shape[4]
        start = length + (block * canvas_ref.shape[3] + b) * thin
        for part in range(2):
            total = None if pair == 0 else canvas_ref[part, k, block, b]
            for w in (2 * pair, 2 * pair + 1):
                piece = moved[w % places, part, k, pl.ds(start - rows_ref[w], thin), :]
                total = piece if total is None else total + piece
            canvas_ref[part, k, block, b] = total

    pairs = count // 2
    enters(0)
    for p in range(pairs):
        a, b = 2 * p, 2 * p + 1
        left(wave, left_ref, half, 0)
        if p:
            halves(leave, back, left_ref, b - 2, 1, 2)
        enters(b)
        left(wave, left_ref, half, 1)
        halves(compare, half, right_ref, a, 0, 2)
        left(chi, right_ref, back, 0)
        if p:
            for block in range(canvas_ref.shape[2]):
                for share in range(canvas_ref.shape[3]):
                    for k in range(spans):
                        place(p - 1, block, share, k)
        halves(compare, half, right_ref, b, 1, 2)
        left(chi, right_ref, back, 1)
        halves(leave, back, left_ref, a, 0, 2)
        enters(a + 2)
    halves(leave, back, left_ref, count - 1, 1, 2)
    return functools.partial(place, pairs - 1)


def combine(
    net, place, entries, positions, canvas_ref, term_ref, misfit_ref,
    step_ref, probe_ref, loss_ref,
    pieces, side, strip, rims, folded, folded_in, grads,
    term_col, term_a, term_in, small, small_col,
):
    beam, beams = net.axes["beam"]
    row, rows_count = net.axes["row"]
    col, cols_count = net.axes["col"]
    blocks = strip.shape[1]
    cols = strip.shape[4]
    beam_peers, col_peers = net.others("beam"), net.others("col")
    order = beam_peers + [beam]
    wide = [(b, r) for b in order for r in net.others("row") + [row]][:-1]
    to = lambda b, r: {"beam": b, "row": r}

    lines = pieces.shape[3]
    for c in range(cols_count):
        for b in range(beams):
            for r in range(rows_count):
                at = ((c * beams + b) * rows_count + r) * lines
                pieces[c, b, r] = term_ref[at // term_ref.shape[1], pl.ds(at % term_ref.shape[1], lines), :]
    term_copies = [net.send({"col": c}, pieces.at[c], term_col.at[k]) for k, c in enumerate(col_peers)]
    across = []
    for p in order:
        for block in range(blocks):
            place(block, p, 0)
            place(block, p, 2)
        across.append(net.sides(
            "col",
            (canvas_ref.at[:, 0, :, p], side.at[1, :, :, p]),
            (canvas_ref.at[:, 2, :, p], side.at[0, :, :, p]),
        ))
    for p in order:
        for block in range(blocks):
            place(block, p, 1)
    for one in term_copies:
        one.wait_recv()
    total = pieces[col]
    for k in range(cols_count - 1):
        total += term_col[k]
    term_a[...] = total
    term_copies = [net.send(to(b, r), term_a.at[b, r], term_in.at[i]) for i, (b, r) in enumerate(wide)]

    along = []
    for i, p in enumerate(order):
        across[i]()
        strip[:, :, p] = canvas_ref[:, 1, :, p] + side[0, :, :, p] + side[1, :, :, p]
        along.append(net.sides(
            "row",
            (strip.at[:, 0, p], rims.at[1, :, p]),
            (strip.at[:, blocks - 1, p], rims.at[0, :, p]),
        ))
    grids = []
    for i, p in enumerate(order):
        along[i]()
        folded[i] = strip[:, 1 : blocks - 1, p]
        folded[i, :, 0] += rims[0, :, p]
        folded[i, :, blocks - 3] += rims[1, :, p]
        if i < beams - 1:
            grids.append(net.send({"beam": p}, folded.at[i], folded_in.at[i]))

    total = term_a[beam, row]
    for i, one in enumerate(term_copies):
        one.wait_recv()
        total += term_in[i]
    probe_ref[col, beam, row] = total * (1.0 / positions)
    mine = probe_ref.at[col, beam, row]
    term_copies = [net.send(to(b, r), mine, mine) for b, r in wide]
    total = folded[beams - 1]
    for i, one in enumerate(grids):
        one.wait_recv()
        total += folded_in[i]
    grads[0, :, beam] = total[0]
    grads[1, :, beam] = -total[1]
    misfit_sum = misfit_ref[:, :cols]
    for k in range(1, misfit_ref.shape[1] // cols):
        misfit_sum += misfit_ref[:, k * cols : (k + 1) * cols]
    small[beam, row, 0] = jnp.sum((total * total).reshape(-1, 8, cols), axis=0)
    small[beam, row, 1] = misfit_sum
    mine = small.at[beam, row]
    smalls = [net.send(to(b, r), mine, mine) for b, r in wide]
    mine = grads.at[:, :, beam]
    grid_copies = [net.send({"beam": p}, mine, mine) for p in beam_peers]
    col_copies = []
    for i, p in enumerate(order):
        for one in term_copies[i * rows_count : (i + 1) * rows_count]:
            one.wait_recv()
        mine = probe_ref.at[col, p]
        col_copies += [net.send({"col": c}, mine, mine) for c in col_peers]
    for one in smalls:
        one.wait_recv()
    total = small[0, 0]
    for k in range(1, beams * rows_count):
        total += small[k // rows_count, k % rows_count]
    small_col[col] = total
    smalls = [net.send({"col": c}, small_col.at[col], small_col.at[col]) for c in col_peers]
    for one in grid_copies + smalls:
        one.wait_recv()
    total = small_col[0]
    for k in range(1, cols_count):
        total += small_col[k]
    mean_square = jnp.sum(total[0], keepdims=True) / entries
    factor = jnp.minimum(1.0, 0.5 / jnp.sqrt(mean_square + 1e-06))
    step_ref[...] = grads[...] * factor[None, None, None]
    loss_ref[...] = jnp.sum(total[1], keepdims=True) * (1.0 / (positions * misfit_ref.shape[1] ** 2))
    for one in col_copies:
        one.wait_recv()
    net.finish()


def whole_kernel(
    sizes, half_length, entries, positions,
    rows_in, cols_in, phase_ref, absorb_ref, probe_in, amplitude_in, left_in, right_in,
    step_ref, probe_out, loss_ref,
    rows_ref, cols_ref, volume, part, slots, trans, probe, amplitude, left, right,
    kept, wave, half, chi, back, moved, canvas, term, misfit,
    pieces, side, strip, rims, folded, folded_in, grads,
    term_col, term_a, term_in, small, small_col,
    load_sem, early_sem, send_sem, recv_sem,
):
    net = Sends(sizes, send_sem, recv_sem)
    col, cols_count = net.axes["col"]
    stages = project(net, half_length, phase_ref, absorb_ref, trans, volume, part, slots, load_sem)
    next(stages)
    early = [
        pltpu.make_async_copy(src, dst, early_sem.at[k])
        for k, (src, dst) in enumerate(
            (
                (rows_in, rows_ref), (cols_in, cols_ref), (probe_in, probe),
                (left_in, left), (amplitude_in, amplitude), (right_in, right),
            )
        )
    ]
    for one in early:
        one.start()
    trans[0] = jnp.ones(trans.shape[1:], jnp.float32)
    trans[1] = jnp.zeros(trans.shape[1:], jnp.float32)
    rims[...] = jnp.zeros_like(rims)
    misfit[...] = jnp.zeros_like(misfit)

    @pl.when(col == 0)
    def _():
        side[0] = jnp.zeros(side.shape[1:], jnp.float32)

    @pl.when(col == cols_count - 1)
    def _():
        side[1] = jnp.zeros(side.shape[1:], jnp.float32)

    length = probe.shape[1]
    blank = jnp.zeros(moved.shape[1:3] + (length, moved.shape[4]), jnp.float32)
    for k in range(moved.shape[0]):
        moved[k, :, :, :length, :] = blank
        moved[k, :, :, 2 * length :, :] = blank
    next(stages)
    for one in early:
        one.wait()
    place = windows(
        rows_ref, cols_ref, trans, probe, amplitude, left, right,
        canvas, term, misfit, kept, wave, half, chi, back, moved,
    )
    combine(
        net, place, entries, positions, canvas, term, misfit, step_ref, probe_out, loss_ref,
        pieces, side, strip, rims, folded, folded_in, grads,
        term_col, term_a, term_in, small, small_col,
    )


def pin(x):
    return pltpu.with_memory_space_constraint(x, pltpu.HBM)


def local(phase_volume, absorb_volume, probe, amplitudes, scan_rows, scan_cols):
    length = probe.shape[1]
    half = length // 2
    count = scan_rows.shape[2]
    depth, rows, cols = phase_volume.shape
    sizes = tuple((axis, lax.axis_size(axis)) for axis in ("beam", "row", "col"))
    counts = dict(sizes)
    beams, rows_count, cols_count = counts["beam"], counts["row"], counts["col"]
    positions = count * beams * rows_count * cols_count
    assert half == cols and count % 2 == 0
    left, right = dft_matrices(length)
    f32, bf16 = jnp.float32, jnp.bfloat16
    share = rows // beams
    tall = rows + 2 * half
    blocks = tall // half
    thin = half // beams
    lines = 2 * length // (cols_count * beams * rows_count)
    shape = (cols_count, beams, rows_count, lines, length)
    grid = (2, blocks - 2, beams, thin, cols)
    entries = 2 * rows * cols * rows_count * cols_count
    wide = beams * rows_count
    wires = 10 * beams + (cols_count + 1) + 2 * beams + wide + 2 * beams + 2 * wide + beams * (cols_count + 1) + cols_count + 16
    vmem = pltpu.VMEM
    hbm = pl.BlockSpec(memory_space=pltpu.HBM)
    step, probe_gradient, loss = pl.pallas_call(
        functools.partial(whole_kernel, sizes, half, entries, positions),
        out_shape=[jax.ShapeDtypeStruct(s, f32) for s in (grid, shape, (1, 1))],
        in_specs=[hbm] * 8,
        out_specs=vmem_specs(3),
        scratch_shapes=[
            pltpu.SMEM((count,), jnp.int32),
            pltpu.SMEM((count,), jnp.int32),
            vmem((2, beams, depth, share, cols), phase_volume.dtype),
            vmem((beams, 2, share, cols), f32),
            vmem((beams - 1, 2, share, cols), f32),
            vmem((2, 3, tall, cols), f32),
            vmem(probe.shape, f32),
            vmem((count, length, length), amplitudes.dtype),
            vmem(left.shape, bf16),
            vmem(right.shape, bf16),
            vmem((2, 2, length, length), f32),
            vmem((2, 2 * length, length), bf16),
            vmem((2, length, 2 * length), bf16),
            vmem((2, 2 * length, length), bf16),
            vmem((2, length, 2 * length), bf16),
            vmem((4, 2, 3, 3 * length, cols), f32),
            vmem((2, 3, blocks, beams, thin, cols), f32),
            vmem(probe.shape, f32),
            vmem((8, length), f32),
            vmem(shape, f32),
            vmem((2, 2, blocks, beams, thin, cols), f32),
            vmem((2, blocks, beams, thin, cols), f32),
            vmem((2, 2, beams, thin, cols), f32),
            vmem((beams, 2, blocks - 2, thin, cols), f32),
            vmem((beams - 1, 2, blocks - 2, thin, cols), f32),
            vmem(grid, f32),
            vmem((cols_count - 1,) + shape[1:], f32),
            vmem(shape[1:], f32),
            vmem((wide - 1,) + shape[3:], f32),
            vmem((beams, rows_count, 2, 8, cols), f32),
            vmem((cols_count, 2, 8, cols), f32),
            pltpu.SemaphoreType.DMA((2, beams)),
            pltpu.SemaphoreType.DMA((6,)),
            pltpu.SemaphoreType.DMA((wires,)),
            pltpu.SemaphoreType.DMA((wires,)),
        ],
        compiler_params=pltpu.CompilerParams(
            collective_id=1, has_side_effects=True, vmem_limit_bytes=48 * 2**20
        ),
    )(
        pin(scan_rows.reshape(count)), pin(scan_cols.reshape(count)), pin(phase_volume), pin(absorb_volume), pin(probe),
        pin(amplitudes.reshape(count, length, length)), pin(left), pin(right),
    )
    return step.reshape(2, rows, cols), probe_gradient.reshape(probe.shape), loss.reshape(())


def solution(mesh):
    in_specs = (
        P("beam", "row", "col"),
        P("beam", "row", "col"),
        P(),
        P("row", "col", "beam", None, None),
        P("row", "col", "beam"),
        P("row", "col", "beam"),
    )
    out_specs = (P(None, "row", "col"), P(), P())
    return jax.shard_map(local, mesh=mesh, in_specs=in_specs, out_specs=out_specs, check_vma=False)
```

```python
import functools
import math

import jax
import jax.numpy as jnp
import numpy as np
from jax import lax
from jax.experimental import pallas as pl
from jax.experimental.pallas import tpu as pltpu
from jax.sharding import PartitionSpec as P


def dft_matrices(length):
    indices = np.arange(length, dtype=np.int32)
    product = indices[:, None] * indices[None, :] % length
    angles = product.astype(np.float32) * np.float32(2.0 * math.pi / length)
    factor = np.float32(1.0 / math.sqrt(length))
    real = (np.cos(angles) * factor).astype(jnp.bfloat16)
    imag = (-np.sin(angles) * factor).astype(jnp.bfloat16)
    left = np.block([[real, -imag], [imag, real]])
    right = np.block([[real, imag], [-imag, real]])
    return jnp.asarray(left), jnp.asarray(right)


def partners(me, count):
    if count % 4 == 0:
        high, low = me // 4 * 4 + me % 4 // 2 * 2, me % 2
        flips = [(1, 1), (0, 1), (1, 0)]
        near = []
        for up, across in flips:
            other = me // 4 * 4 + lax.rem(me % 4 // 2 + up, 2) * 2 + lax.rem(low + across, 2)
            near.append(other)
        if count == 4:
            return near
    return [lax.rem(me + d, count) for d in range(1, count)]


class Sends:
    def __init__(self, sizes, send_sem, recv_sem):
        self.axes = {axis: (lax.axis_index(axis), count) for axis, count in sizes}
        self.sends, self.recvs = send_sem, recv_sem
        self.used = self.base = 0
        self.started = []

    def greet(self):
        self.barrier = pltpu.get_barrier_semaphore()
        targets = [{axis: other} for axis in self.axes for other in self.others(axis)]
        for target in targets:
            pl.semaphore_signal(self.barrier, inc=1, device_id=target, device_id_type=pl.DeviceIdType.MESH)
        return lambda: pl.semaphore_wait(self.barrier, len(targets))

    def others(self, axis):
        return partners(*self.axes[axis])

    def take(self):
        self.used += 1
        return self.used - 1

    def copy(self, target, src, dst, index=None):
        index = self.take() if index is None else index
        return pltpu.make_async_remote_copy(
            src_ref=src, dst_ref=dst, send_sem=self.sends.at[index - self.base],
            recv_sem=self.recvs.at[index], device_id=target,
            device_id_type=pl.DeviceIdType.MESH,
        )

    def send(self, target, src, dst):
        one = self.copy(target, src, dst)
        one.start()
        self.started.append(one.wait_send)
        return one

    def group(self, targets, src, slots):
        index = self.take()
        for k, target in enumerate(targets):
            self.copy(target, src, slots.at[k], index).start()
        self.started.append(pltpu.make_async_copy(slots, slots, self.sends.at[index - self.base]).wait)
        return pltpu.make_async_copy(slots, slots, self.recvs.at[index]).wait

    def sides(self, axis, down, up, to_before=True, to_after=True, one_way=False, index=None):
        me, count = self.axes[axis]
        both = jnp.logical_and
        sends_before, sends_after = both(me > 0, to_before), both(me < count - 1, to_after)
        gets_after, gets_before = both(me < count - 1, to_before), both(me > 0, to_after)
        index = self.take() if index is None else index
        before = self.copy({axis: lax.rem(me + count - 1, count)}, *down, index)
        after = self.copy({axis: lax.rem(me + 1, count)}, *up, index if one_way or count == 2 else self.take())
        pl.when(sends_before)(before.start)
        pl.when(sends_after)(after.start)

        def wait_send():
            pl.when(sends_before)(before.wait_send)
            pl.when(sends_after)(after.wait_send)

        def wait_recv():
            pl.when(gets_after)(before.wait_recv)
            pl.when(gets_before)(after.wait_recv)

        self.started.append(wait_send)
        return wait_recv

    def finish(self):
        for wait_send in self.started:
            wait_send()
        self.started = []
        self.base = self.used


def tree(values):
    if len(values) == 4:
        return (values[3] + values[1]) + (values[2] + values[0])
    return functools.reduce(lambda a, b: a + b, values)


def vmem_specs(count):
    return [pl.BlockSpec(memory_space=pltpu.VMEM)] * count


def project(net, half, phase_ref, absorb_ref, out_ref, volume, part, slots, load_sem):
    beam, beams = net.axes["beam"]
    row, rows_count = net.axes["row"]
    depth, rows, cols = phase_ref.shape
    share = rows // beams
    edge = half // share
    blocks = rows // share + 2 * edge
    one_way = 2 * edge <= beams
    peers = net.others("beam")
    order = peers + [beam]
    for i, peer in enumerate(order):
        here = pl.ds(pl.multiple_of(peer * share, share), share)
        for plane, ref in enumerate((phase_ref, absorb_ref)):
            pltpu.make_async_copy(ref.at[:, here, :], volume.at[i, plane], load_sem.at[i]).start()
    arrived = net.greet()
    yield
    scatter = []
    for i, peer in enumerate(order):
        pltpu.make_async_copy(volume.at[i], volume.at[i], load_sem.at[i]).wait()
        for plane in range(2):
            total = volume[i, plane, 0].astype(jnp.float32)
            for d in range(1, depth):
                total += volume[i, plane, d].astype(jnp.float32)
            part[i, plane] = total
        if i == 0:
            arrived()
        if i < beams - 1:
            scatter.append(net.send({"beam": peer}, part.at[i], slots.at[i]))
    total = part[beams - 1]
    for i, one in enumerate(scatter):
        one.wait_recv()
        total += slots[i]
    at = lambda side, block: out_ref.at[:, side, pl.ds(pl.multiple_of(block * share, share), share), :]
    damping = jnp.exp(-total[1])
    own = edge + beam
    here = pl.ds(pl.multiple_of(own * share, share), share)
    out_ref[0, 1, here, :] = damping * jnp.cos(total[0])
    out_ref[1, 1, here, :] = damping * jnp.sin(total[0])
    arrivals = []

    def across(block, when=True, index=None):
        arrivals.append(net.sides(
            "col", (at(1, block), at(2, block)), (at(1, block), at(0, block)), when, when, index=index
        ))

    def along(share_at):
        here = at(1, edge + share_at)
        below = lax.rem(edge + beams + share_at, blocks)
        above = lax.rem(edge + share_at + blocks - beams, blocks)
        wait = net.sides(
            "row", (here, at(1, below)), (here, at(1, above)), share_at < edge, share_at >= beams - edge,
            one_way=one_way,
        )
        return wait, share_at, below, above

    gather = [net.send({"beam": peer}, at(1, own), at(1, own)) for peer in peers]
    rims = [along(beam)]
    across(own)
    for peer, one in zip(peers, gather):
        one.wait_recv()
        rims.append(along(peer))
        across(edge + peer)
    for wait, share_at, below, above in rims:
        wait()
        index = net.used if one_way and net.axes["col"][1] == 2 else None
        across(below, jnp.logical_and(row < rows_count - 1, share_at < edge))
        across(above, jnp.logical_and(row > 0, share_at >= beams - edge), index)
    for wait in arrivals:
        wait()
    net.finish()
    yield


def windows(
    rows_ref, cols_ref, trans_ref, probe_ref, amplitude_ref, left_ref, right_ref,
    canvas_ref, term_ref, misfit_ref, kept, wave, half, chi, back, moved,
):
    count, length = amplitude_ref.shape[:2]
    lanes = trans_ref.shape[3]
    spans = trans_ref.shape[1]
    inner = length // lanes
    step = 32
    steps = length // step
    dot = functools.partial(jnp.dot, preferred_element_type=jnp.float32)
    lane = lax.broadcasted_iota(jnp.int32, (step, lanes), 1)
    places = moved.shape[0]

    def enter(w, slot, m):
        row_at, col_at = rows_ref[w], cols_ref[w]
        shift = lax.rem(lanes - col_at, lanes)
        keep = lane < lanes - col_at
        here = pl.ds(m * step, step)
        planes = []
        for part in range(2):
            turned = [
                pltpu.roll(trans_ref[part, k, pl.ds(row_at + m * step, step), :], shift, 1)
                for k in range(spans)
            ]
            planes.append([jnp.where(keep, turned[k], turned[k + 1]) for k in range(inner)])
        for k in range(inner):
            real, imag = planes[0][k], planes[1][k]
            at = pl.ds(k * lanes, lanes)
            probe_real, probe_imag = probe_ref[0, here, at], probe_ref[1, here, at]
            kept[slot, 0, here, at] = real
            kept[slot, 1, here, at] = imag
            wave[slot, pl.ds(m * step, step), at] = (probe_real * real - probe_imag * imag).astype(jnp.bfloat16)
            wave[slot, pl.ds(length + m * step, step), at] = (probe_real * imag + probe_imag * real).astype(jnp.bfloat16)

    def compare(w, slot, m, far):
        here = pl.ds(m, step)
        real, imag = far[:, :length], far[:, length:]
        amplitude = amplitude_ref[w, here, :].astype(jnp.float32)
        square = real * real + imag * imag
        inverse = lax.rsqrt(jnp.maximum(square, 1.2e-38))
        off = square * inverse - amplitude
        misfit_ref[...] += jnp.sum((off * off).reshape(step // 8, 8, length), axis=0)
        ratio = 1.0 - amplitude * jnp.minimum(inverse, 2.0)
        chi[slot, here, :] = (real * ratio).astype(jnp.bfloat16)
        chi[slot, pl.ds(length + m, step), :] = (imag * ratio).astype(jnp.bfloat16)

    def leave(w, slot, m, grad):
        col_at = cols_ref[w]
        here, low = pl.ds(m, step), pl.ds(length + m, step)
        first = lane >= col_at
        objects = [[], []]
        for k in range(inner):
            at = pl.ds(k * lanes, lanes)
            grad_real = grad[:, k * lanes : (k + 1) * lanes]
            grad_imag = grad[:, length + k * lanes : length + (k + 1) * lanes]
            real, imag = kept[slot, 0, here, at], kept[slot, 1, here, at]
            term_real = real * grad_real + imag * grad_imag
            term_imag = real * grad_imag - imag * grad_real
            if w == 0:
                term_ref[here, at] = term_real
                term_ref[low, at] = term_imag
            else:
                term_ref[here, at] += term_real
                term_ref[low, at] += term_imag
            probe_real, probe_imag = probe_ref[0, here, at], probe_ref[1, here, at]
            objects[0].append(pltpu.roll(probe_real * term_imag - probe_imag * term_real, col_at, 1))
            objects[1].append(pltpu.roll(probe_real * term_real + probe_imag * term_imag, col_at, 1))
        for part in range(2):
            turned = objects[part]
            for k in range(spans):
                before = turned[k - 1] if k > 0 else 0.0
                after = turned[k] if k < inner else 0.0
                moved[w % places, part, k, pl.ds(length + m, step), :] = jnp.where(first, after, before)

    def left(values, first, out, slot):
        part = dot(first[...], values[slot])
        out[slot, :, :length] = part[:length].astype(jnp.bfloat16)
        out[slot, :, length:] = part[length:].astype(jnp.bfloat16)

    def halves(make, source, table, w, slot, cut):
        tall = length // cut
        for c in range(cut):
            out = dot(source[slot, c * tall : (c + 1) * tall], table[...])
            for m in range(tall // step):
                make(w, slot, c * tall + m * step, out[m * step : (m + 1) * step])

    def enters(w):
        if w < count:
            for m in range(steps):
                enter(w, w % 2, m)

    def place(pair, block, b, k):
        thin = canvas_ref.shape[4]
        start = length + (block * canvas_ref.shape[3] + b) * thin
        for part in range(2):
            total = None if pair == 0 else canvas_ref[part, k, block, b]
            for w in (2 * pair, 2 * pair + 1):
                piece = moved[w % places, part, k, pl.ds(start - rows_ref[w], thin), :]
                total = piece if total is None else total + piece
            canvas_ref[part, k, block, b] = total

    pairs = count // 2
    enters(0)
    for p in range(pairs):
        a, b = 2 * p, 2 * p + 1
        left(wave, left_ref, half, 0)
        if p:
            halves(leave, back, left_ref, b - 2, 1, 2)
        enters(b)
        left(wave, left_ref, half, 1)
        halves(compare, half, right_ref, a, 0, 2)
        left(chi, right_ref, back, 0)
        if p:
            for block in range(canvas_ref.shape[2]):
                for share in range(canvas_ref.shape[3]):
                    for k in range(spans):
                        place(p - 1, block, share, k)
        halves(compare, half, right_ref, b, 1, 2)
        left(chi, right_ref, back, 1)
        halves(leave, back, left_ref, a, 0, 2)
        enters(a + 2)
    halves(leave, back, left_ref, count - 1, 1, 2)
    return functools.partial(place, pairs - 1)


def combine(
    net, place, entries, positions, canvas_ref, term_ref, misfit_ref,
    step_ref, probe_ref, loss_ref,
    side, strip, rims, folded, folded_in, grads,
    term_col, term_a, term_beam, term_b, term_row, small, small_in, small_all,
):
    beam, beams = net.axes["beam"]
    row, rows_count = net.axes["row"]
    col, cols_count = net.axes["col"]
    blocks = strip.shape[1]
    cols = strip.shape[4]
    lines = term_b.shape[0]
    beam_peers, row_peers, col_peers = (net.others(axis) for axis in ("beam", "row", "col"))
    order = beam_peers + [beam]
    wide = [{"beam": b, "row": r} for b in order for r in row_peers + [row]][:-1]
    rows_of = lambda c, b, n: pl.ds(pl.multiple_of((c * beams + b) * lines, lines), n * lines)

    term_copies = [
        net.send({"col": c}, term_ref.at[rows_of(c, 0, beams), :], term_col.at[k])
        for k, c in enumerate(col_peers)
    ]
    across = []
    for p in order:
        for block in range(blocks):
            place(block, p, 0)
            place(block, p, 2)
        across.append(net.sides(
            "col",
            (canvas_ref.at[:, 0, :, p], side.at[1, :, :, p]),
            (canvas_ref.at[:, 2, :, p], side.at[0, :, :, p]),
        ))
    for p in order:
        for block in range(blocks):
            place(block, p, 1)
    for one in term_copies:
        one.wait_recv()
    term_beams = []
    for i, p in enumerate(order):
        total = term_ref[rows_of(col, p, 1), :]
        for k in range(cols_count - 1):
            total += term_col[k, pl.ds(pl.multiple_of(p * lines, lines), lines), :]
        term_a[i] = total
        if i < beams - 1:
            term_beams.append(net.send({"beam": p}, term_a.at[i], term_beam.at[i]))

    along = []
    for i, p in enumerate(order):
        across[i]()
        strip[:, :, p] = canvas_ref[:, 1, :, p] + side[0, :, :, p] + side[1, :, :, p]
        along.append(net.sides(
            "row",
            (strip.at[:, 0, p], rims.at[1, :, p]),
            (strip.at[:, blocks - 1, p], rims.at[0, :, p]),
        ))
    grids = []
    for i, p in enumerate(order):
        along[i]()
        folded[i] = strip[:, 1 : blocks - 1, p]
        folded[i, :, 0] += rims[0, :, p]
        folded[i, :, blocks - 3] += rims[1, :, p]
        if i < beams - 1:
            grids.append(net.send({"beam": p}, folded.at[i], folded_in.at[i]))

    total = term_a[beams - 1]
    for i, one in enumerate(term_beams):
        one.wait_recv()
        total += term_beam[i]
    term_b[...] = total
    term_rows = [net.send({"row": r}, term_b, term_row.at[k]) for k, r in enumerate(row_peers)]

    total = folded[beams - 1]
    for i, one in enumerate(grids):
        one.wait_recv()
        total += folded_in[i]
    grads[0, :, beam] = total[0]
    grads[1, :, beam] = -total[1]
    misfit_sum = misfit_ref[:, :cols]
    for k in range(1, misfit_ref.shape[1] // cols):
        misfit_sum += misfit_ref[:, k * cols : (k + 1) * cols]
    small[0] = jnp.sum((total * total).reshape(-1, 8, cols), axis=0)
    small[1] = misfit_sum
    small_wait = net.group(wide, small, small_in)
    mine = grads.at[:, :, beam]
    grid_copies = [net.send({"beam": p}, mine, mine) for p in beam_peers]

    for one in term_rows:
        one.wait_recv()
    total = tree([term_row[k] for k in range(rows_count - 1)] + [term_b[...]])
    probe_ref[rows_of(col, beam, 1), :] = total * (1.0 / positions)
    share = lambda p: probe_ref.at[rows_of(col, p, 1), :]
    term_copies = [net.send({"beam": p}, share(beam), share(beam)) for p in beam_peers]
    col_copies = [net.send({"col": c}, share(beam), share(beam)) for c in col_peers]
    small_wait()
    sums = [small_in[k] for k in range(beams * rows_count - 1)] + [small[...]]
    small_all[col] = tree([tree(sums[b * rows_count : (b + 1) * rows_count]) for b in range(beams)])
    smalls = [net.send({"col": c}, small_all.at[col], small_all.at[col]) for c in col_peers]
    for p, one in zip(beam_peers, term_copies):
        one.wait_recv()
        col_copies += [net.send({"col": c}, share(p), share(p)) for c in col_peers]
    for one in grid_copies + smalls:
        one.wait_recv()
    total = small_all[0]
    for k in range(1, cols_count):
        total += small_all[k]
    mean_square = jnp.sum(total[0], keepdims=True) / entries
    factor = jnp.minimum(1.0, 0.5 / jnp.sqrt(mean_square + 1e-06))
    step_ref[...] = grads[...] * factor[None, None, None]
    loss_ref[...] = jnp.sum(total[1], keepdims=True) * (1.0 / (positions * misfit_ref.shape[1] ** 2))
    for one in col_copies:
        one.wait_recv()
    net.finish()
    assert net.used == net.recvs.shape[0]


def whole_kernel(
    sizes, half_length, entries, positions,
    rows_in, cols_in, phase_ref, absorb_ref, probe_in, amplitude_in, left_in, right_in,
    step_ref, probe_out, loss_ref,
    rows_ref, cols_ref, volume, part, slots, trans, probe, amplitude, left, right,
    kept, wave, half, chi, back, moved, canvas, term, misfit,
    side, strip, rims, folded, folded_in, grads,
    term_col, term_a, term_beam, term_b, term_row, small, small_in, small_all,
    load_sem, early_sem, send_sem, recv_sem,
):
    net = Sends(sizes, send_sem, recv_sem)
    row, rows_count = net.axes["row"]
    col, cols_count = net.axes["col"]
    stages = project(net, half_length, phase_ref, absorb_ref, trans, volume, part, slots, load_sem)
    next(stages)
    early = [
        pltpu.make_async_copy(src, dst, early_sem.at[k])
        for k, (src, dst) in enumerate(
            (
                (rows_in, rows_ref), (cols_in, cols_ref), (probe_in, probe),
                (left_in, left), (amplitude_in, amplitude), (right_in, right),
            )
        )
    ]
    for one in early:
        one.start()
    misfit[...] = jnp.zeros_like(misfit)

    def empty(where):
        trans[(0,) + where] = jnp.ones_like(trans[(0,) + where])
        trans[(1,) + where] = jnp.zeros_like(trans[(1,) + where])

    for k, at in ((0, 0), (1, cols_count - 1)):

        @pl.when(col == at)
        def _():
            side[k] = jnp.zeros(side.shape[1:], jnp.float32)
            empty((2 * k,))

    for k, at in ((0, 0), (1, rows_count - 1)):

        @pl.when(row == at)
        def _():
            rims[k] = jnp.zeros(rims.shape[1:], jnp.float32)
            begin = k * (trans.shape[2] - half_length)
            for j in range(3):
                empty((j, pl.ds(begin, half_length)))

    length = probe.shape[1]
    blank = jnp.zeros(moved.shape[1:3] + (length, moved.shape[4]), jnp.float32)
    for k in range(moved.shape[0]):
        moved[k, :, :, :length, :] = blank
        moved[k, :, :, 2 * length :, :] = blank
    next(stages)
    for one in early:
        one.wait()
    place = windows(
        rows_ref, cols_ref, trans, probe, amplitude, left, right,
        canvas, term, misfit, kept, wave, half, chi, back, moved,
    )
    combine(
        net, place, entries, positions, canvas, term, misfit, step_ref, probe_out, loss_ref,
        side, strip, rims, folded, folded_in, grads,
        term_col, term_a, term_beam, term_b, term_row, small, small_in, small_all,
    )


def pin(x):
    return pltpu.with_memory_space_constraint(x, pltpu.HBM)


def local(phase_volume, absorb_volume, probe, amplitudes, scan_rows, scan_cols):
    length = probe.shape[1]
    half = length // 2
    count = scan_rows.shape[2]
    depth, rows, cols = phase_volume.shape
    sizes = tuple((axis, lax.axis_size(axis)) for axis in ("beam", "row", "col"))
    counts = dict(sizes)
    beams, rows_count, cols_count = counts["beam"], counts["row"], counts["col"]
    positions = count * beams * rows_count * cols_count
    assert half == cols and count % 2 == 0
    left, right = dft_matrices(length)
    f32, bf16 = jnp.float32, jnp.bfloat16
    share = rows // beams
    tall = rows + 2 * half
    blocks = tall // half
    thin = half // beams
    chunk = 2 * length // cols_count
    lines = chunk // beams
    grid = (2, blocks - 2, beams, thin, cols)
    entries = 2 * rows * cols * rows_count * cols_count
    ways = 1 if cols_count == 2 else 2
    one_way = 2 * half <= rows
    early = 2 * (beams - 1) + (1 if one_way else 2) * beams
    early += beams * (2 if one_way and ways == 1 else 3 * ways)
    late = (cols_count - 1) * (2 + beams) + (ways + 2) * beams + 4 * (beams - 1) + rows_count
    vmem = pltpu.VMEM
    hbm = pl.BlockSpec(memory_space=pltpu.HBM)
    step, probe_gradient, loss = pl.pallas_call(
        functools.partial(whole_kernel, sizes, half, entries, positions),
        out_shape=[jax.ShapeDtypeStruct(s, f32) for s in (grid, (2 * length, length), (1, 1))],
        in_specs=[hbm] * 8,
        out_specs=vmem_specs(3),
        scratch_shapes=[
            pltpu.SMEM((count,), jnp.int32),
            pltpu.SMEM((count,), jnp.int32),
            vmem((beams, 2, depth, share, cols), phase_volume.dtype),
            vmem((beams, 2, share, cols), f32),
            vmem((beams - 1, 2, share, cols), f32),
            vmem((2, 3, tall, cols), f32),
            vmem(probe.shape, f32),
            vmem((count, length, length), amplitudes.dtype),
            vmem(left.shape, bf16),
            vmem(right.shape, bf16),
            vmem((2, 2, length, length), f32),
            vmem((2, 2 * length, length), bf16),
            vmem((2, length, 2 * length), bf16),
            vmem((2, 2 * length, length), bf16),
            vmem((2, length, 2 * length), bf16),
            vmem((4, 2, 3, 3 * length, cols), f32),
            vmem((2, 3, blocks, beams, thin, cols), f32),
            vmem((2 * length, length), f32),
            vmem((8, length), f32),
            vmem((2, 2, blocks, beams, thin, cols), f32),
            vmem((2, blocks, beams, thin, cols), f32),
            vmem((2, 2, beams, thin, cols), f32),
            vmem((beams, 2, blocks - 2, thin, cols), f32),
            vmem((beams - 1, 2, blocks - 2, thin, cols), f32),
            vmem(grid, f32),
            vmem((cols_count - 1, chunk, length), f32),
            vmem((beams, lines, length), f32),
            vmem((beams - 1, lines, length), f32),
            vmem((lines, length), f32),
            vmem((rows_count - 1, lines, length), f32),
            vmem((2, 8, cols), f32),
            vmem((beams * rows_count - 1, 2, 8, cols), f32),
            vmem((cols_count, 2, 8, cols), f32),
            pltpu.SemaphoreType.DMA((beams,)),
            pltpu.SemaphoreType.DMA((6,)),
            pltpu.SemaphoreType.DMA((max(early, late),)),
            pltpu.SemaphoreType.DMA((early + late,)),
        ],
        compiler_params=pltpu.CompilerParams(
            collective_id=1, has_side_effects=True, vmem_limit_bytes=48 * 2**20
        ),
    )(
        pin(scan_rows.reshape(count)), pin(scan_cols.reshape(count)), pin(phase_volume), pin(absorb_volume), pin(probe),
        pin(amplitudes.reshape(count, length, length)), pin(left), pin(right),
    )
    return step.reshape(2, rows, cols), probe_gradient.reshape(probe.shape), loss.reshape(())


def solution(mesh):
    in_specs = (
        P("beam", "row", "col"),
        P("beam", "row", "col"),
        P(),
        P("row", "col", "beam", None, None),
        P("row", "col", "beam"),
        P("row", "col", "beam"),
    )
    out_specs = (P(None, "row", "col"), P(), P())
    return jax.shard_map(local, mesh=mesh, in_specs=in_specs, out_specs=out_specs, check_vma=False)
```

```python
import functools
import math

import jax
import jax.numpy as jnp
import numpy as np
from jax import lax
from jax.experimental import pallas as pl
from jax.experimental.pallas import tpu as pltpu
from jax.sharding import PartitionSpec as P


def dft_matrices(length):
    indices = np.arange(length, dtype=np.int32)
    product = indices[:, None] * indices[None, :] % length
    angles = product.astype(np.float32) * np.float32(2.0 * math.pi / length)
    factor = np.float32(1.0 / math.sqrt(length))
    real = (np.cos(angles) * factor).astype(jnp.bfloat16)
    imag = (-np.sin(angles) * factor).astype(jnp.bfloat16)
    left = np.block([[real, -imag], [imag, real]])
    right = np.block([[real, imag], [-imag, real]])
    return jnp.asarray(left), jnp.asarray(right)


def partners(me, count):
    if count % 4 == 0:
        high, low = me // 4 * 4 + me % 4 // 2 * 2, me % 2
        flips = [(1, 1), (0, 1), (1, 0)]
        near = []
        for up, across in flips:
            other = me // 4 * 4 + lax.rem(me % 4 // 2 + up, 2) * 2 + lax.rem(low + across, 2)
            near.append(other)
        if count == 4:
            return near
    return [lax.rem(me + d, count) for d in range(1, count)]


class Sends:
    def __init__(self, sizes, send_sem, recv_sem):
        self.axes = {axis: (lax.axis_index(axis), count) for axis, count in sizes}
        self.sends, self.recvs = send_sem, recv_sem
        self.used = self.base = 0
        self.started = []

    def greet(self):
        self.barrier = pltpu.get_barrier_semaphore()
        targets = [{axis: other} for axis in self.axes for other in self.others(axis)]
        for target in targets:
            pl.semaphore_signal(self.barrier, inc=1, device_id=target, device_id_type=pl.DeviceIdType.MESH)
        return lambda: pl.semaphore_wait(self.barrier, len(targets))

    def others(self, axis):
        return partners(*self.axes[axis])

    def take(self):
        self.used += 1
        return self.used - 1

    def copy(self, target, src, dst, index=None):
        index = self.take() if index is None else index
        return pltpu.make_async_remote_copy(
            src_ref=src, dst_ref=dst, send_sem=self.sends.at[index - self.base],
            recv_sem=self.recvs.at[index], device_id=target,
            device_id_type=pl.DeviceIdType.MESH,
        )

    def send(self, target, src, dst):
        one = self.copy(target, src, dst)
        one.start()
        self.started.append(one.wait_send)
        return one

    def group(self, targets, src, slots):
        index = self.take()
        for k, target in enumerate(targets):
            self.copy(target, src, slots.at[k], index).start()
        self.started.append(pltpu.make_async_copy(slots, slots, self.sends.at[index - self.base]).wait)
        return pltpu.make_async_copy(slots, slots, self.recvs.at[index]).wait

    def sides(self, axis, down, up, to_before=True, to_after=True, one_way=False, index=None):
        me, count = self.axes[axis]
        both = jnp.logical_and
        sends_before, sends_after = both(me > 0, to_before), both(me < count - 1, to_after)
        gets_after, gets_before = both(me < count - 1, to_before), both(me > 0, to_after)
        index = self.take() if index is None else index
        before = self.copy({axis: lax.rem(me + count - 1, count)}, *down, index)
        after = self.copy({axis: lax.rem(me + 1, count)}, *up, index if one_way or count == 2 else self.take())
        pl.when(sends_before)(before.start)
        pl.when(sends_after)(after.start)

        def wait_send():
            pl.when(sends_before)(before.wait_send)
            pl.when(sends_after)(after.wait_send)

        def wait_recv():
            pl.when(gets_after)(before.wait_recv)
            pl.when(gets_before)(after.wait_recv)

        self.started.append(wait_send)
        return wait_recv

    def finish(self):
        for wait_send in self.started:
            wait_send()
        self.started = []
        self.base = self.used


def tree(values):
    if len(values) == 4:
        return (values[3] + values[1]) + (values[2] + values[0])
    return functools.reduce(lambda a, b: a + b, values)


def vmem_specs(count):
    return [pl.BlockSpec(memory_space=pltpu.VMEM)] * count


def project(net, half, phase_ref, absorb_ref, out_ref, volume, part, slots, load_sem):
    beam, beams = net.axes["beam"]
    row, rows_count = net.axes["row"]
    depth, rows, cols = phase_ref.shape
    share = rows // beams
    edge = half // share
    blocks = rows // share + 2 * edge
    one_way = 2 * edge <= beams
    peers = net.others("beam")
    order = peers + [beam]
    for i, peer in enumerate(order):
        here = pl.ds(pl.multiple_of(peer * share, share), share)
        for plane, ref in enumerate((phase_ref, absorb_ref)):
            pltpu.make_async_copy(ref.at[:, here, :], volume.at[i, plane], load_sem.at[i]).start()
    arrived = net.greet()
    yield
    scatter = []
    for i, peer in enumerate(order):
        pltpu.make_async_copy(volume.at[i], volume.at[i], load_sem.at[i]).wait()
        for plane in range(2):
            total = volume[i, plane, 0].astype(jnp.float32)
            for d in range(1, depth):
                total += volume[i, plane, d].astype(jnp.float32)
            part[i, plane] = total
        if i == 0:
            arrived()
        if i < beams - 1:
            scatter.append(net.send({"beam": peer}, part.at[i], slots.at[i]))
    total = part[beams - 1]
    for i, one in enumerate(scatter):
        one.wait_recv()
        total += slots[i]
    at = lambda side, block: out_ref.at[:, side, pl.ds(pl.multiple_of(block * share, share), share), :]
    damping = jnp.exp(-total[1])
    own = edge + beam
    here = pl.ds(pl.multiple_of(own * share, share), share)
    out_ref[0, 1, here, :] = damping * jnp.cos(total[0])
    out_ref[1, 1, here, :] = damping * jnp.sin(total[0])
    arrivals = []

    def across(block, when=True, index=None):
        arrivals.append(net.sides(
            "col", (at(1, block), at(2, block)), (at(1, block), at(0, block)), when, when, index=index
        ))

    def rim_blocks(share_at):
        return lax.rem(edge + beams + share_at, blocks), lax.rem(edge + share_at + blocks - beams, blocks)

    def rim_here(share_at):
        from_after = jnp.logical_and(row < rows_count - 1, share_at < edge)
        from_before = jnp.logical_and(row > 0, share_at >= beams - edge)
        return from_after, from_before

    def along():
        below, above = rim_blocks(beam)
        wait = net.sides(
            "row", (at(1, own), at(1, below)), (at(1, own), at(1, above)), beam < edge, beam >= beams - edge,
            one_way=one_way,
        )
        return wait, below, above

    def around(peer, share_at):
        waits = []
        index = net.take()
        for block, here, there in zip(rim_blocks(share_at), rim_here(share_at), rim_here(peer)):
            one = net.copy({"beam": peer}, at(1, block), at(1, block), index)
            pl.when(here)(one.start)
            net.started.append(functools.partial(pl.when(here), one.wait_send))
            waits.append(functools.partial(pl.when(there), one.wait_recv))
            index = index if one_way or waits[1:] else net.take()
        return lambda: [wait() for wait in waits]

    def spread(share_at, below, above):
        from_after, from_before = rim_here(share_at)
        index = net.used if one_way and net.axes["col"][1] == 2 else None
        across(below, from_after)
        across(above, from_before, index)

    wait_rim, below, above = along()
    gather = [net.send({"beam": peer}, at(1, own), at(1, own)) for peer in peers]
    across(own)
    wait_rim()
    rims = [around(peer, beam) for peer in peers]
    spread(beam, below, above)
    for peer, one in zip(peers, gather):
        one.wait_recv()
        across(edge + peer)
    for peer, wait in zip(peers, rims):
        wait()
        spread(peer, *rim_blocks(peer))
    for wait in arrivals:
        wait()
    net.finish()
    yield


def windows(
    rows_ref, cols_ref, trans_ref, probe_ref, amplitude_ref, left_ref, right_ref,
    canvas_ref, term_ref, misfit_ref, kept, wave, half, chi, back, moved,
):
    count, length = amplitude_ref.shape[:2]
    lanes = trans_ref.shape[3]
    spans = trans_ref.shape[1]
    inner = length // lanes
    step = 32
    steps = length // step
    dot = functools.partial(jnp.dot, preferred_element_type=jnp.float32)
    lane = lax.broadcasted_iota(jnp.int32, (step, lanes), 1)
    places = moved.shape[0]

    def enter(w, slot, m):
        row_at, col_at = rows_ref[w], cols_ref[w]
        shift = lax.rem(lanes - col_at, lanes)
        keep = lane < lanes - col_at
        here = pl.ds(m * step, step)
        planes = []
        for part in range(2):
            turned = [
                pltpu.roll(trans_ref[part, k, pl.ds(row_at + m * step, step), :], shift, 1)
                for k in range(spans)
            ]
            planes.append([jnp.where(keep, turned[k], turned[k + 1]) for k in range(inner)])
        for k in range(inner):
            real, imag = planes[0][k], planes[1][k]
            at = pl.ds(k * lanes, lanes)
            probe_real, probe_imag = probe_ref[0, here, at], probe_ref[1, here, at]
            kept[slot, 0, here, at] = real
            kept[slot, 1, here, at] = imag
            wave[slot, pl.ds(m * step, step), at] = (probe_real * real - probe_imag * imag).astype(jnp.bfloat16)
            wave[slot, pl.ds(length + m * step, step), at] = (probe_real * imag + probe_imag * real).astype(jnp.bfloat16)

    def compare(w, slot, m, far):
        here = pl.ds(m, step)
        real, imag = far[:, :length], far[:, length:]
        amplitude = amplitude_ref[w, here, :].astype(jnp.float32)
        square = real * real + imag * imag
        inverse = lax.rsqrt(jnp.maximum(square, 1.2e-38))
        off = square * inverse - amplitude
        misfit_ref[...] += jnp.sum((off * off).reshape(step // 8, 8, length), axis=0)
        ratio = 1.0 - amplitude * jnp.minimum(inverse, 2.0)
        chi[slot, here, :] = (real * ratio).astype(jnp.bfloat16)
        chi[slot, pl.ds(length + m, step), :] = (imag * ratio).astype(jnp.bfloat16)

    def leave(w, slot, m, grad):
        col_at = cols_ref[w]
        here, low = pl.ds(m, step), pl.ds(length + m, step)
        first = lane >= col_at
        objects = [[], []]
        for k in range(inner):
            at = pl.ds(k * lanes, lanes)
            grad_real = grad[:, k * lanes : (k + 1) * lanes]
            grad_imag = grad[:, length + k * lanes : length + (k + 1) * lanes]
            real, imag = kept[slot, 0, here, at], kept[slot, 1, here, at]
            term_real = real * grad_real + imag * grad_imag
            term_imag = real * grad_imag - imag * grad_real
            if w == 0:
                term_ref[here, at] = term_real
                term_ref[low, at] = term_imag
            else:
                term_ref[here, at] += term_real
                term_ref[low, at] += term_imag
            probe_real, probe_imag = probe_ref[0, here, at], probe_ref[1, here, at]
            objects[0].append(pltpu.roll(probe_real * term_imag - probe_imag * term_real, col_at, 1))
            objects[1].append(pltpu.roll(probe_real * term_real + probe_imag * term_imag, col_at, 1))
        for part in range(2):
            turned = objects[part]
            for k in range(spans):
                before = turned[k - 1] if k > 0 else 0.0
                after = turned[k] if k < inner else 0.0
                moved[w % places, part, k, pl.ds(length + m, step), :] = jnp.where(first, after, before)

    def left(values, first, out, slot):
        part = dot(first[...], values[slot])
        out[slot, :, :length] = part[:length].astype(jnp.bfloat16)
        out[slot, :, length:] = part[length:].astype(jnp.bfloat16)

    def halves(make, source, table, w, slot, cut):
        tall = length // cut
        for c in range(cut):
            out = dot(source[slot, c * tall : (c + 1) * tall], table[...])
            for m in range(tall // step):
                make(w, slot, c * tall + m * step, out[m * step : (m + 1) * step])

    def enters(w):
        if w < count:
            for m in range(steps):
                enter(w, w % 2, m)

    def place(pair, block, b, k):
        thin = canvas_ref.shape[4]
        start = length + (block * canvas_ref.shape[3] + b) * thin
        for part in range(2):
            total = None if pair == 0 else canvas_ref[part, k, block, b]
            for w in (2 * pair, 2 * pair + 1):
                piece = moved[w % places, part, k, pl.ds(start - rows_ref[w], thin), :]
                total = piece if total is None else total + piece
            canvas_ref[part, k, block, b] = total

    pairs = count // 2
    enters(0)
    for p in range(pairs):
        a, b = 2 * p, 2 * p + 1
        left(wave, left_ref, half, 0)
        if p:
            halves(leave, back, left_ref, b - 2, 1, 2)
        enters(b)
        left(wave, left_ref, half, 1)
        halves(compare, half, right_ref, a, 0, 2)
        left(chi, right_ref, back, 0)
        if p:
            for block in range(canvas_ref.shape[2]):
                for share in range(canvas_ref.shape[3]):
                    for k in range(spans):
                        place(p - 1, block, share, k)
        halves(compare, half, right_ref, b, 1, 2)
        left(chi, right_ref, back, 1)
        halves(leave, back, left_ref, a, 0, 2)
        enters(a + 2)
    halves(leave, back, left_ref, count - 1, 1, 2)
    return functools.partial(place, pairs - 1)


def combine(
    net, place, entries, positions, canvas_ref, term_ref, misfit_ref,
    step_ref, probe_ref, loss_ref,
    side, strip, rims, folded, folded_in, grads,
    term_col, term_a, term_beam, term_b, term_row, small, small_in, small_all,
):
    beam, beams = net.axes["beam"]
    row, rows_count = net.axes["row"]
    col, cols_count = net.axes["col"]
    blocks = strip.shape[1]
    cols = strip.shape[4]
    lines = term_b.shape[0]
    beam_peers, row_peers, col_peers = (net.others(axis) for axis in ("beam", "row", "col"))
    order = beam_peers + [beam]
    wide = [{"beam": b, "row": r} for b in order for r in row_peers + [row]][:-1]
    rows_of = lambda c, b, n: pl.ds(pl.multiple_of((c * beams + b) * lines, lines), n * lines)

    term_copies = [
        net.send({"col": c}, term_ref.at[rows_of(c, 0, beams), :], term_col.at[k])
        for k, c in enumerate(col_peers)
    ]
    across = []
    for p in order:
        for block in range(blocks):
            place(block, p, 0)
            place(block, p, 2)
        across.append(net.sides(
            "col",
            (canvas_ref.at[:, 0, :, p], side.at[1, :, :, p]),
            (canvas_ref.at[:, 2, :, p], side.at[0, :, :, p]),
        ))
    for p in order:
        for block in range(blocks):
            place(block, p, 1)
    for one in term_copies:
        one.wait_recv()
    term_beams = []
    for i, p in enumerate(order):
        total = term_ref[rows_of(col, p, 1), :]
        for k in range(cols_count - 1):
            total += term_col[k, pl.ds(pl.multiple_of(p * lines, lines), lines), :]
        term_a[i] = total
        if i < beams - 1:
            term_beams.append(net.send({"beam": p}, term_a.at[i], term_beam.at[i]))

    along = []
    for i, p in enumerate(order):
        across[i]()
        strip[:, :, p] = canvas_ref[:, 1, :, p] + side[0, :, :, p] + side[1, :, :, p]
        along.append(net.sides(
            "row",
            (strip.at[:, 0, p], rims.at[1, :, p]),
            (strip.at[:, blocks - 1, p], rims.at[0, :, p]),
        ))
    grids = []
    for i, p in enumerate(order):
        along[i]()
        folded[i] = strip[:, 1 : blocks - 1, p]
        folded[i, :, 0] += rims[0, :, p]
        folded[i, :, blocks - 3] += rims[1, :, p]
        if i < beams - 1:
            grids.append(net.send({"beam": p}, folded.at[i], folded_in.at[i]))

    total = term_a[beams - 1]
    for i, one in enumerate(term_beams):
        one.wait_recv()
        total += term_beam[i]
    term_b[...] = total
    term_rows = [net.send({"row": r}, term_b, term_row.at[k]) for k, r in enumerate(row_peers)]

    total = folded[beams - 1]
    for i, one in enumerate(grids):
        one.wait_recv()
        total += folded_in[i]
    grads[0, :, beam] = total[0]
    grads[1, :, beam] = -total[1]
    misfit_sum = misfit_ref[:, :cols]
    for k in range(1, misfit_ref.shape[1] // cols):
        misfit_sum += misfit_ref[:, k * cols : (k + 1) * cols]
    small[0] = jnp.sum((total * total).reshape(-1, 8, cols), axis=0)
    small[1] = misfit_sum
    small_wait = net.group(wide, small, small_in)
    mine = grads.at[:, :, beam]
    grid_copies = [net.send({"beam": p}, mine, mine) for p in beam_peers]

    for one in term_rows:
        one.wait_recv()
    total = tree([term_row[k] for k in range(rows_count - 1)] + [term_b[...]])
    probe_ref[rows_of(col, beam, 1), :] = total * (1.0 / positions)
    share = lambda p: probe_ref.at[rows_of(col, p, 1), :]
    term_copies = [net.send({"beam": p}, share(beam), share(beam)) for p in beam_peers]
    col_copies = [net.send({"col": c}, share(beam), share(beam)) for c in col_peers]
    small_wait()
    sums = [small_in[k] for k in range(beams * rows_count - 1)] + [small[...]]
    small_all[col] = tree([tree(sums[b * rows_count : (b + 1) * rows_count]) for b in range(beams)])
    smalls = [net.send({"col": c}, small_all.at[col], small_all.at[col]) for c in col_peers]
    for p, one in zip(beam_peers, term_copies):
        one.wait_recv()
        col_copies += [net.send({"col": c}, share(p), share(p)) for c in col_peers]
    for one in grid_copies + smalls:
        one.wait_recv()
    total = small_all[0]
    for k in range(1, cols_count):
        total += small_all[k]
    mean_square = jnp.sum(total[0], keepdims=True) / entries
    factor = jnp.minimum(1.0, 0.5 / jnp.sqrt(mean_square + 1e-06))
    step_ref[...] = grads[...] * factor[None, None, None]
    loss = jnp.sum(total[1], keepdims=True) * (1.0 / (positions * misfit_ref.shape[1] ** 2))
    loss_ref[...] = jnp.broadcast_to(loss, loss_ref.shape)
    for one in col_copies:
        one.wait_recv()
    net.finish()
    assert net.used == net.recvs.shape[0]


def whole_kernel(
    sizes, half_length, entries, positions,
    rows_in, cols_in, phase_ref, absorb_ref, probe_in, amplitude_in, left_in, right_in,
    step_ref, probe_out, loss_ref,
    rows_ref, cols_ref, volume, part, slots, trans, probe, amplitude, left, right,
    kept, wave, half, chi, back, moved, canvas, term, misfit,
    side, strip, rims, folded, folded_in, grads,
    term_col, term_a, term_beam, term_b, term_row, small, small_in, small_all,
    load_sem, early_sem, send_sem, recv_sem,
):
    net = Sends(sizes, send_sem, recv_sem)
    row, rows_count = net.axes["row"]
    col, cols_count = net.axes["col"]
    stages = project(net, half_length, phase_ref, absorb_ref, trans, volume, part, slots, load_sem)
    next(stages)
    early = [
        pltpu.make_async_copy(src, dst, early_sem.at[k])
        for k, (src, dst) in enumerate(
            (
                (rows_in, rows_ref), (cols_in, cols_ref), (probe_in, probe),
                (left_in, left), (amplitude_in, amplitude), (right_in, right),
            )
        )
    ]
    for one in early:
        one.start()
    misfit[...] = jnp.zeros_like(misfit)

    def empty(where):
        trans[(0,) + where] = jnp.ones_like(trans[(0,) + where])
        trans[(1,) + where] = jnp.zeros_like(trans[(1,) + where])

    for k, at in ((0, 0), (1, cols_count - 1)):

        @pl.when(col == at)
        def _():
            side[k] = jnp.zeros(side.shape[1:], jnp.float32)
            empty((2 * k,))

    for k, at in ((0, 0), (1, rows_count - 1)):

        @pl.when(row == at)
        def _():
            rims[k] = jnp.zeros(rims.shape[1:], jnp.float32)
            begin = k * (trans.shape[2] - half_length)
            for j in range(3):
                empty((j, pl.ds(begin, half_length)))

    length = probe.shape[1]
    blank = jnp.zeros(moved.shape[1:3] + (length, moved.shape[4]), jnp.float32)
    for k in range(moved.shape[0]):
        moved[k, :, :, :length, :] = blank
        moved[k, :, :, 2 * length :, :] = blank
    next(stages)
    for one in early:
        one.wait()
    place = windows(
        rows_ref, cols_ref, trans, probe, amplitude, left, right,
        canvas, term, misfit, kept, wave, half, chi, back, moved,
    )
    combine(
        net, place, entries, positions, canvas, term, misfit, step_ref, probe_out, loss_ref,
        side, strip, rims, folded, folded_in, grads,
        term_col, term_a, term_beam, term_b, term_row, small, small_in, small_all,
    )


def close_kernel(step_in, probe_in, loss_in, step_ref, probe_ref, loss_ref, one, sems):
    copies = [
        pltpu.make_async_copy(src, dst, sems.at[k])
        for k, (src, dst) in enumerate(((probe_in, probe_ref), (step_in, step_ref), (one, loss_ref)))
    ]
    copies[0].start()
    copies[1].start()
    one[...] = loss_in[:1, :1]
    copies[2].start()
    for copy in copies:
        copy.wait()


def pin(x):
    return pltpu.with_memory_space_constraint(x, pltpu.HBM)


def local(phase_volume, absorb_volume, probe, amplitudes, scan_rows, scan_cols):
    length = probe.shape[1]
    half = length // 2
    count = scan_rows.shape[2]
    depth, rows, cols = phase_volume.shape
    sizes = tuple((axis, lax.axis_size(axis)) for axis in ("beam", "row", "col"))
    counts = dict(sizes)
    beams, rows_count, cols_count = counts["beam"], counts["row"], counts["col"]
    positions = count * beams * rows_count * cols_count
    assert half == cols and count % 2 == 0
    left, right = dft_matrices(length)
    f32, bf16 = jnp.float32, jnp.bfloat16
    share = rows // beams
    tall = rows + 2 * half
    blocks = tall // half
    thin = half // beams
    chunk = 2 * length // cols_count
    lines = chunk // beams
    grid = (2, blocks - 2, beams, thin, cols)
    entries = 2 * rows * cols * rows_count * cols_count
    ways = 1 if cols_count == 2 else 2
    one_way = 2 * half <= rows
    early = 2 * (beams - 1) + (1 if one_way else 2) * beams
    early += beams * (2 if one_way and ways == 1 else 3 * ways)
    late = (cols_count - 1) * (2 + beams) + (ways + 2) * beams + 4 * (beams - 1) + rows_count
    vmem = pltpu.VMEM
    hbm = pl.BlockSpec(memory_space=pltpu.HBM)
    step, probe_gradient, loss = pl.pallas_call(
        functools.partial(whole_kernel, sizes, half, entries, positions),
        out_shape=[jax.ShapeDtypeStruct(s, f32) for s in (grid, (2 * length, length), (8, cols))],
        in_specs=[hbm] * 8,
        out_specs=vmem_specs(3),
        scratch_shapes=[
            pltpu.SMEM((count,), jnp.int32),
            pltpu.SMEM((count,), jnp.int32),
            vmem((beams, 2, depth, share, cols), phase_volume.dtype),
            vmem((beams, 2, share, cols), f32),
            vmem((beams - 1, 2, share, cols), f32),
            vmem((2, 3, tall, cols), f32),
            vmem(probe.shape, f32),
            vmem((count, length, length), amplitudes.dtype),
            vmem(left.shape, bf16),
            vmem(right.shape, bf16),
            vmem((2, 2, length, length), f32),
            vmem((2, 2 * length, length), bf16),
            vmem((2, length, 2 * length), bf16),
            vmem((2, 2 * length, length), bf16),
            vmem((2, length, 2 * length), bf16),
            vmem((4, 2, 3, 3 * length, cols), f32),
            vmem((2, 3, blocks, beams, thin, cols), f32),
            vmem((2 * length, length), f32),
            vmem((8, length), f32),
            vmem((2, 2, blocks, beams, thin, cols), f32),
            vmem((2, blocks, beams, thin, cols), f32),
            vmem((2, 2, beams, thin, cols), f32),
            vmem((beams, 2, blocks - 2, thin, cols), f32),
            vmem((beams - 1, 2, blocks - 2, thin, cols), f32),
            vmem(grid, f32),
            vmem((cols_count - 1, chunk, length), f32),
            vmem((beams, lines, length), f32),
            vmem((beams - 1, lines, length), f32),
            vmem((lines, length), f32),
            vmem((rows_count - 1, lines, length), f32),
            vmem((2, 8, cols), f32),
            vmem((beams * rows_count - 1, 2, 8, cols), f32),
            vmem((cols_count, 2, 8, cols), f32),
            pltpu.SemaphoreType.DMA((beams,)),
            pltpu.SemaphoreType.DMA((6,)),
            pltpu.SemaphoreType.DMA((max(early, late),)),
            pltpu.SemaphoreType.DMA((early + late,)),
        ],
        compiler_params=pltpu.CompilerParams(
            collective_id=1, has_side_effects=True, vmem_limit_bytes=48 * 2**20
        ),
    )(
        pin(scan_rows.reshape(count)), pin(scan_cols.reshape(count)), pin(phase_volume), pin(absorb_volume), pin(probe),
        pin(amplitudes.reshape(count, length, length)), pin(left), pin(right),
    )
    step, probe_gradient, loss = pl.pallas_call(
        close_kernel,
        out_shape=[jax.ShapeDtypeStruct(s, f32) for s in (grid, (2 * length, length), (1, 1))],
        in_specs=vmem_specs(3),
        out_specs=[hbm] * 3,
        scratch_shapes=[vmem((1, 1), f32), pltpu.SemaphoreType.DMA((3,))],
        compiler_params=pltpu.CompilerParams(vmem_limit_bytes=2**20),
    )(step, probe_gradient, loss)
    return step.reshape(2, rows, cols), probe_gradient.reshape(probe.shape), loss.reshape(())


def solution(mesh):
    in_specs = (
        P("beam", "row", "col"),
        P("beam", "row", "col"),
        P(),
        P("row", "col", "beam", None, None),
        P("row", "col", "beam"),
        P("row", "col", "beam"),
    )
    out_specs = (P(None, "row", "col"), P(), P())
    return jax.shard_map(local, mesh=mesh, in_specs=in_specs, out_specs=out_specs, check_vma=False)
```

```python
import functools
import math

import jax
import jax.numpy as jnp
import numpy as np
from jax import lax
from jax.experimental import pallas as pl
from jax.experimental.pallas import tpu as pltpu
from jax.sharding import PartitionSpec as P


def dft_matrices(length):
    indices = np.arange(length, dtype=np.int32)
    product = indices[:, None] * indices[None, :] % length
    angles = product.astype(np.float32) * np.float32(2.0 * math.pi / length)
    factor = np.float32(1.0 / math.sqrt(length))
    real = (np.cos(angles) * factor).astype(jnp.bfloat16)
    imag = (-np.sin(angles) * factor).astype(jnp.bfloat16)
    left = np.block([[real, -imag], [imag, real]])
    right = np.block([[real, imag], [-imag, real]])
    return jnp.asarray(left), jnp.asarray(right)


def partners(me, count):
    if count == 4:
        flips = ((1, 1), (0, 1), (1, 0))
        return [lax.rem(me // 2 + up, 2) * 2 + lax.rem(me % 2 + across, 2) for up, across in flips]
    return [lax.rem(me + d, count) for d in range(1, count)]


class Sends:
    def __init__(self, sizes, send_sem, recv_sem):
        self.axes = {axis: (lax.axis_index(axis), count) for axis, count in sizes}
        self.sends, self.recvs = send_sem, recv_sem
        self.used = self.base = 0
        self.started = []

    def greet(self):
        self.barrier = pltpu.get_barrier_semaphore()
        targets = [{axis: other} for axis in self.axes for other in self.others(axis)]
        for target in targets:
            pl.semaphore_signal(self.barrier, inc=1, device_id=target, device_id_type=pl.DeviceIdType.MESH)
        return lambda: pl.semaphore_wait(self.barrier, len(targets))

    def others(self, axis):
        return partners(*self.axes[axis])

    def take(self):
        self.used += 1
        return self.used - 1

    def copy(self, target, src, dst, index=None):
        index = self.take() if index is None else index
        return pltpu.make_async_remote_copy(
            src_ref=src, dst_ref=dst, send_sem=self.sends.at[index - self.base],
            recv_sem=self.recvs.at[index], device_id=target,
            device_id_type=pl.DeviceIdType.MESH,
        )

    def send(self, target, src, dst):
        one = self.copy(target, src, dst)
        one.start()
        self.started.append(one.wait_send)
        return one

    def group(self, targets, src, slots):
        index = self.take()
        for k, target in enumerate(targets):
            self.copy(target, src, slots.at[k], index).start()
        self.started.append(pltpu.make_async_copy(slots, slots, self.sends.at[index - self.base]).wait)
        return pltpu.make_async_copy(slots, slots, self.recvs.at[index]).wait

    def sides(self, axis, down, up, to_before=True, to_after=True, one_way=False, index=None):
        me, count = self.axes[axis]
        both = jnp.logical_and
        sends_before, sends_after = both(me > 0, to_before), both(me < count - 1, to_after)
        gets_after, gets_before = both(me < count - 1, to_before), both(me > 0, to_after)
        index = self.take() if index is None else index
        before = self.copy({axis: lax.rem(me + count - 1, count)}, *down, index)
        after = self.copy({axis: lax.rem(me + 1, count)}, *up, index if one_way or count == 2 else self.take())
        pl.when(sends_before)(before.start)
        pl.when(sends_after)(after.start)

        def wait_send():
            pl.when(sends_before)(before.wait_send)
            pl.when(sends_after)(after.wait_send)

        def wait_recv():
            pl.when(gets_after)(before.wait_recv)
            pl.when(gets_before)(after.wait_recv)

        self.started.append(wait_send)
        return wait_recv

    def finish(self):
        for wait_send in self.started:
            wait_send()
        self.started = []
        self.base = self.used


def tree(values):
    if len(values) == 4:
        return (values[3] + values[1]) + (values[2] + values[0])
    return functools.reduce(lambda a, b: a + b, values)


def vmem_specs(count):
    return [pl.BlockSpec(memory_space=pltpu.VMEM)] * count


def project(net, half, phase_ref, absorb_ref, out_ref, volume, part, slots, load_sem):
    beam, beams = net.axes["beam"]
    row, rows_count = net.axes["row"]
    depth, rows, cols = phase_ref.shape
    share = rows // beams
    edge = half // share
    blocks = rows // share + 2 * edge
    one_way = 2 * edge <= beams
    peers = net.others("beam")
    order = peers + [beam]
    for i, peer in enumerate(order):
        here = pl.ds(pl.multiple_of(peer * share, share), share)
        for plane, ref in enumerate((phase_ref, absorb_ref)):
            pltpu.make_async_copy(ref.at[:, here, :], volume.at[i, plane], load_sem.at[i]).start()
    arrived = net.greet()
    yield
    scatter = []
    for i, peer in enumerate(order):
        pltpu.make_async_copy(volume.at[i], volume.at[i], load_sem.at[i]).wait()
        for plane in range(2):
            total = volume[i, plane, 0].astype(jnp.float32)
            for d in range(1, depth):
                total += volume[i, plane, d].astype(jnp.float32)
            part[i, plane] = total
        if i == 0:
            arrived()
        if i < beams - 1:
            scatter.append(net.send({"beam": peer}, part.at[i], slots.at[i]))
    yield
    total = part[beams - 1]
    for i, one in enumerate(scatter):
        one.wait_recv()
        total += slots[i]
    at = lambda side, block: out_ref.at[:, side, pl.ds(pl.multiple_of(block * share, share), share), :]
    damping = jnp.exp(-total[1])
    own = edge + beam
    here = pl.ds(pl.multiple_of(own * share, share), share)
    out_ref[0, 1, here, :] = damping * jnp.cos(total[0])
    out_ref[1, 1, here, :] = damping * jnp.sin(total[0])
    arrivals = []

    def across(block, when=True, index=None):
        arrivals.append(net.sides(
            "col", (at(1, block), at(2, block)), (at(1, block), at(0, block)), when, when, index=index
        ))

    def rim_blocks(share_at):
        return lax.rem(edge + beams + share_at, blocks), lax.rem(edge + share_at + blocks - beams, blocks)

    def rim_here(share_at):
        from_after = jnp.logical_and(row < rows_count - 1, share_at < edge)
        from_before = jnp.logical_and(row > 0, share_at >= beams - edge)
        return from_after, from_before

    def along():
        below, above = rim_blocks(beam)
        wait = net.sides(
            "row", (at(1, own), at(1, below)), (at(1, own), at(1, above)), beam < edge, beam >= beams - edge,
            one_way=one_way,
        )
        return wait, below, above

    def around(peer, share_at):
        waits = []
        index = net.take()
        for block, here, there in zip(rim_blocks(share_at), rim_here(share_at), rim_here(peer)):
            one = net.copy({"beam": peer}, at(1, block), at(1, block), index)
            pl.when(here)(one.start)
            net.started.append(functools.partial(pl.when(here), one.wait_send))
            waits.append(functools.partial(pl.when(there), one.wait_recv))
            index = index if one_way or waits[1:] else net.take()
        return lambda: [wait() for wait in waits]

    def spread(share_at, below, above):
        from_after, from_before = rim_here(share_at)
        index = net.used if one_way and net.axes["col"][1] == 2 else None
        across(below, from_after)
        across(above, from_before, index)

    wait_rim, below, above = along()
    gather = [net.send({"beam": peer}, at(1, own), at(1, own)) for peer in peers]
    across(own)
    wait_rim()
    rims = [around(peer, beam) for peer in peers]
    spread(beam, below, above)
    for peer, one in zip(peers, gather):
        one.wait_recv()
        across(edge + peer)
    for peer, wait in zip(peers, rims):
        wait()
        spread(peer, *rim_blocks(peer))
    for wait in arrivals:
        wait()
    net.finish()
    yield


def windows(
    rows_ref, cols_ref, trans_ref, probe_ref, amplitude_ref, left_ref, right_ref,
    canvas_ref, term_ref, misfit_ref, kept, wave, half, chi, back, moved,
):
    count, length = amplitude_ref.shape[:2]
    lanes = trans_ref.shape[3]
    spans = trans_ref.shape[1]
    inner = length // lanes
    step = 32
    steps = length // step
    dot = functools.partial(jnp.dot, preferred_element_type=jnp.float32)
    lane = lax.broadcasted_iota(jnp.int32, (step, lanes), 1)
    places = moved.shape[0]

    def enter(w, slot, m):
        row_at, col_at = rows_ref[w], cols_ref[w]
        shift = lax.rem(lanes - col_at, lanes)
        keep = lane < lanes - col_at
        here = pl.ds(m * step, step)
        planes = []
        for part in range(2):
            turned = [
                pltpu.roll(trans_ref[part, k, pl.ds(row_at + m * step, step), :], shift, 1)
                for k in range(spans)
            ]
            planes.append([jnp.where(keep, turned[k], turned[k + 1]) for k in range(inner)])
        for k in range(inner):
            real, imag = planes[0][k], planes[1][k]
            at = pl.ds(k * lanes, lanes)
            probe_real, probe_imag = probe_ref[0, here, at], probe_ref[1, here, at]
            kept[slot, 0, here, at] = real
            kept[slot, 1, here, at] = imag
            wave[slot, pl.ds(m * step, step), at] = (probe_real * real - probe_imag * imag).astype(jnp.bfloat16)
            wave[slot, pl.ds(length + m * step, step), at] = (probe_real * imag + probe_imag * real).astype(jnp.bfloat16)

    def compare(w, slot, m, far):
        here = pl.ds(m, step)
        real, imag = far[:, :length], far[:, length:]
        amplitude = amplitude_ref[w, here, :].astype(jnp.float32)
        square = real * real + imag * imag
        inverse = lax.rsqrt(jnp.maximum(square, 1.2e-38))
        off = square * inverse - amplitude
        misfit_ref[...] += jnp.sum((off * off).reshape(step // 8, 8, length), axis=0)
        ratio = 1.0 - amplitude * jnp.minimum(inverse, 2.0)
        chi[slot, here, :] = (real * ratio).astype(jnp.bfloat16)
        chi[slot, pl.ds(length + m, step), :] = (imag * ratio).astype(jnp.bfloat16)

    def leave(w, slot, m, grad):
        col_at = cols_ref[w]
        here, low = pl.ds(m, step), pl.ds(length + m, step)
        first = lane >= col_at
        objects = [[], []]
        for k in range(inner):
            at = pl.ds(k * lanes, lanes)
            grad_real = grad[:, k * lanes : (k + 1) * lanes]
            grad_imag = grad[:, length + k * lanes : length + (k + 1) * lanes]
            real, imag = kept[slot, 0, here, at], kept[slot, 1, here, at]
            term_real = real * grad_real + imag * grad_imag
            term_imag = real * grad_imag - imag * grad_real
            if w == 0:
                term_ref[here, at] = term_real
                term_ref[low, at] = term_imag
            else:
                term_ref[here, at] += term_real
                term_ref[low, at] += term_imag
            probe_real, probe_imag = probe_ref[0, here, at], probe_ref[1, here, at]
            objects[0].append(pltpu.roll(probe_real * term_imag - probe_imag * term_real, col_at, 1))
            objects[1].append(pltpu.roll(probe_real * term_real + probe_imag * term_imag, col_at, 1))
        for part in range(2):
            turned = objects[part]
            for k in range(spans):
                before = turned[k - 1] if k > 0 else 0.0
                after = turned[k] if k < inner else 0.0
                moved[w % places, part, k, pl.ds(length + m, step), :] = jnp.where(first, after, before)

    def left(values, first, out, slot):
        for k in range(2):
            part = dot(first[pl.ds(k * length, length), :], values[slot])
            out[slot, :, k * length : (k + 1) * length] = part.astype(jnp.bfloat16)

    def halves(make, source, table, w, slot, cut):
        tall = length // cut
        for c in range(cut):
            out = dot(source[slot, c * tall : (c + 1) * tall], table[...])
            for m in range(tall // step):
                make(w, slot, c * tall + m * step, out[m * step : (m + 1) * step])

    def enters(w):
        if w < count:
            for m in range(steps):
                enter(w, w % slots, m)

    def forth(w):
        if w < count:
            left(wave, left_ref, half, w % slots)

    def judge(w):
        if w < count:
            halves(compare, half, right_ref, w, w % slots, 1)

    def backs(w):
        if w < count:
            left(chi, right_ref, back, w % slots)

    def leaves(w):
        if 0 <= w < count:
            halves(leave, back, left_ref, w, w % slots, 1)

    def place(pair, block, b, k):
        thin = canvas_ref.shape[4]
        start = length + (block * canvas_ref.shape[3] + b) * thin
        for part in range(2):
            total = None if pair == 0 else canvas_ref[part, k, block, b]
            for w in (2 * pair, 2 * pair + 1):
                piece = moved[w % places, part, k, pl.ds(start - rows_ref[w], thin), :]
                total = piece if total is None else total + piece
            canvas_ref[part, k, block, b] = total

    def settle(pair):
        if 0 <= pair < pairs - 1:
            for block in range(canvas_ref.shape[2]):
                for share in range(canvas_ref.shape[3]):
                    for k in range(spans):
                        place(pair, block, share, k)

    slots = kept.shape[0]
    pairs = count // 2
    enters(0)
    enters(1)
    forth(0)
    for w in range(count):
        enters(w + 2)
        judge(w)
        forth(w + 1)
        leaves(w - 1)
        backs(w)
        if w % 2 == 0:
            settle(w // 2 - 1)
    leaves(count - 1)
    return functools.partial(place, pairs - 1)


def combine(
    net, place, entries, positions, canvas_ref, term_ref, misfit_ref,
    step_ref, probe_ref, loss_ref,
    side, strip, rims, folded, folded_in, grads,
    term_col, term_a, term_beam, term_b, term_row, small, small_in, small_all,
):
    beam, beams = net.axes["beam"]
    row, rows_count = net.axes["row"]
    col, cols_count = net.axes["col"]
    blocks = strip.shape[1]
    cols = strip.shape[4]
    thin = term_b.shape[1]
    lines = rows_count * thin
    beam_peers, row_peers, col_peers = (net.others(axis) for axis in ("beam", "row", "col"))
    order = beam_peers + [beam]
    row_order = row_peers[::2] + row_peers[1::2] + [row]
    wide = [{"beam": b, "row": r} for b in order for r in row_peers + [row]][:-1]
    rows_of = lambda c, b, n: pl.ds(pl.multiple_of((c * beams + b) * lines, lines), n * lines)

    term_copies = [
        net.send({"col": c}, term_ref.at[rows_of(c, 0, beams), :], term_col.at[k])
        for k, c in enumerate(col_peers)
    ]
    across = []
    for p in order:
        for block in range(blocks):
            place(block, p, 0)
            place(block, p, 2)
        across.append(net.sides(
            "col",
            (canvas_ref.at[:, 0, :, p], side.at[1, :, :, p]),
            (canvas_ref.at[:, 2, :, p], side.at[0, :, :, p]),
        ))
    for p in order:
        for block in range(blocks):
            place(block, p, 1)
    for one in term_copies:
        one.wait_recv()
    for i, p in enumerate(order):
        total = term_ref[rows_of(col, p, 1), :]
        for k in range(cols_count - 1):
            total += term_col[k, pl.ds(pl.multiple_of(p * lines, lines), lines), :]
        for r in range(rows_count):
            term_a[i, r] = total[r * thin : (r + 1) * thin]
    term_beams = []
    for r in row_order:
        index = net.take()
        slots = term_beam.at[r]
        for i, p in enumerate(beam_peers):
            net.copy({"beam": p}, term_a.at[i, r], slots.at[i], index).start()
        net.started.append(pltpu.make_async_copy(slots, slots, net.sends.at[index - net.base]).wait)
        term_beams.append(pltpu.make_async_copy(slots, slots, net.recvs.at[index]).wait)

    along = []
    for i, p in enumerate(order):
        across[i]()
        strip[:, :, p] = canvas_ref[:, 1, :, p] + side[0, :, :, p] + side[1, :, :, p]
        along.append(net.sides(
            "row",
            (strip.at[:, 0, p], rims.at[1, :, p]),
            (strip.at[:, blocks - 1, p], rims.at[0, :, p]),
        ))
    grids = []

    def fold(i, p):
        along[i]()
        folded[i] = strip[:, 1 : blocks - 1, p]
        folded[i, :, 0] += rims[0, :, p]
        folded[i, :, blocks - 3] += rims[1, :, p]
        if i < beams - 1:
            grids.append(net.send({"beam": p}, folded.at[i], folded_in.at[i]))

    term_rows = []

    def gather(k, r):
        term_beams[k]()
        total = term_a[beams - 1, r]
        for i in range(beams - 1):
            total += term_beam[r, i]
        term_b[r] = total
        if k < rows_count - 1:
            term_rows.append(net.send({"row": r}, term_b.at[r], term_row.at[k]))

    for i, p in enumerate(order):
        fold(i, p)
        if i < rows_count:
            gather(i, row_order[i])
    for k in range(beams, rows_count):
        gather(k, row_order[k])

    total = term_b[row]
    for k, one in enumerate(term_rows):
        one.wait_recv()
        total += term_row[k]
    probe_ref[col, beam, row] = total * (1.0 / positions)
    piece = lambda r: probe_ref.at[col, beam, r]
    term_rows = [net.send({"row": r}, piece(row), piece(row)) for r in row_peers]
    around = [net.take() for _ in beam_peers]

    def forward(r):
        for p, index in zip(beam_peers, around):
            net.copy({"beam": p}, piece(r), piece(r), index).start()

    forward(row)

    total = folded[beams - 1]
    for i, one in enumerate(grids):
        one.wait_recv()
        total += folded_in[i]
    grads[0, :, beam] = total[0]
    grads[1, :, beam] = -total[1]
    misfit_sum = misfit_ref[:, :cols]
    for k in range(1, misfit_ref.shape[1] // cols):
        misfit_sum += misfit_ref[:, k * cols : (k + 1) * cols]
    small[:1] = jnp.sum((total * total).reshape(-1, cols), axis=0, keepdims=True)
    small[1:] = jnp.sum(misfit_sum, axis=0, keepdims=True)
    small_wait = net.group(wide, small, small_in)
    mine = grads.at[:, :, beam]
    grid_copies = [net.send({"beam": p}, mine, mine) for p in beam_peers]

    for r, one in zip(row_peers, term_rows):
        one.wait_recv()
        forward(r)
    share = lambda p: probe_ref.at[col, p]
    for index in around:
        net.started.append(pltpu.make_async_copy(share(beam), share(beam), net.sends.at[index - net.base]).wait)
    col_copies = [net.send({"col": c}, share(beam), share(beam)) for c in col_peers]
    small_wait()
    sums = [small_in[k] for k in range(beams * rows_count - 1)] + [small[...]]
    small_all[col] = tree([tree(sums[b * rows_count : (b + 1) * rows_count]) for b in range(beams)])
    smalls = [net.send({"col": c}, small_all.at[col], small_all.at[col]) for c in col_peers]
    for p, index in zip(beam_peers, around):
        pltpu.make_async_copy(share(p), share(p), net.recvs.at[index]).wait()
        col_copies += [net.send({"col": c}, share(p), share(p)) for c in col_peers]
    for one in grid_copies + smalls:
        one.wait_recv()
    total = small_all[0]
    for k in range(1, cols_count):
        total += small_all[k]
    mean_square = jnp.sum(total[:1], keepdims=True) / entries
    factor = jnp.minimum(1.0, 0.5 / jnp.sqrt(mean_square + 1e-06))
    step_ref[...] = grads[...] * factor[None, None, None]
    loss = jnp.sum(total[1:], keepdims=True) * (1.0 / (positions * misfit_ref.shape[1] ** 2))
    loss_ref[...] = jnp.broadcast_to(loss, loss_ref.shape)
    for one in col_copies:
        one.wait_recv()
    net.finish()
    assert net.used == net.recvs.shape[0]


def whole_kernel(
    sizes, half_length, entries, positions,
    rows_in, cols_in, phase_ref, absorb_ref, probe_in, amplitude_in, left_in, right_in,
    step_ref, probe_out, loss_ref,
    rows_ref, cols_ref, volume, part, slots, trans, probe, amplitude, left, right,
    kept, wave, half, chi, back, moved, canvas, term, misfit,
    side, strip, rims, folded, folded_in, grads,
    term_col, term_a, term_beam, term_b, term_row, small, small_in, small_all,
    load_sem, early_sem, send_sem, recv_sem,
):
    net = Sends(sizes, send_sem, recv_sem)
    row, rows_count = net.axes["row"]
    col, cols_count = net.axes["col"]
    stages = project(net, half_length, phase_ref, absorb_ref, trans, volume, part, slots, load_sem)
    next(stages)
    early = [
        pltpu.make_async_copy(src, dst, early_sem.at[k])
        for k, (src, dst) in enumerate(
            (
                (rows_in, rows_ref), (cols_in, cols_ref), (probe_in, probe),
                (left_in, left), (amplitude_in, amplitude), (right_in, right),
            )
        )
    ]
    misfit[...] = jnp.zeros_like(misfit)

    def empty(where):
        trans[(0,) + where] = jnp.ones_like(trans[(0,) + where])
        trans[(1,) + where] = jnp.zeros_like(trans[(1,) + where])

    for k, at in ((0, 0), (1, cols_count - 1)):

        @pl.when(col == at)
        def _():
            side[k] = jnp.zeros(side.shape[1:], jnp.float32)
            empty((2 * k,))

    for k, at in ((0, 0), (1, rows_count - 1)):

        @pl.when(row == at)
        def _():
            rims[k] = jnp.zeros(rims.shape[1:], jnp.float32)
            begin = k * (trans.shape[2] - half_length)
            for j in range(3):
                empty((j, pl.ds(begin, half_length)))

    length = probe.shape[1]
    blank = jnp.zeros(moved.shape[1:3] + (length, moved.shape[4]), jnp.float32)
    for k in range(moved.shape[0]):
        moved[k, :, :, :length, :] = blank
        moved[k, :, :, 2 * length :, :] = blank
    next(stages)
    for one in early:
        one.start()
    next(stages)
    for one in early:
        one.wait()
    place = windows(
        rows_ref, cols_ref, trans, probe, amplitude, left, right,
        canvas, term, misfit, kept, wave, half, chi, back, moved,
    )
    combine(
        net, place, entries, positions, canvas, term, misfit, step_ref, probe_out, loss_ref,
        side, strip, rims, folded, folded_in, grads,
        term_col, term_a, term_beam, term_b, term_row, small, small_in, small_all,
    )


def close_kernel(step_in, probe_in, loss_in, step_ref, probe_ref, loss_ref, one, sems):
    copies = [
        pltpu.make_async_copy(src, dst, sems.at[k])
        for k, (src, dst) in enumerate(((probe_in, probe_ref), (step_in, step_ref), (one, loss_ref)))
    ]
    copies[0].start()
    copies[1].start()
    one[...] = loss_in[:1, :1]
    copies[2].start()
    for copy in copies:
        copy.wait()


def pin(x):
    return pltpu.with_memory_space_constraint(x, pltpu.HBM)


def local(phase_volume, absorb_volume, probe, amplitudes, scan_rows, scan_cols):
    length = probe.shape[1]
    half = length // 2
    count = scan_rows.shape[2]
    depth, rows, cols = phase_volume.shape
    sizes = tuple((axis, lax.axis_size(axis)) for axis in ("beam", "row", "col"))
    counts = dict(sizes)
    beams, rows_count, cols_count = counts["beam"], counts["row"], counts["col"]
    positions = count * beams * rows_count * cols_count
    assert half == cols and count % 2 == 0
    left, right = dft_matrices(length)
    f32, bf16 = jnp.float32, jnp.bfloat16
    share = rows // beams
    tall = rows + 2 * half
    blocks = tall // half
    thin = half // beams
    chunk = 2 * length // cols_count
    lines = chunk // beams
    pieces = (cols_count, beams, rows_count, lines // rows_count, length)
    grid = (2, blocks - 2, beams, thin, cols)
    entries = 2 * rows * cols * rows_count * cols_count
    ways = 1 if cols_count == 2 else 2
    one_way = 2 * half <= rows
    early = 2 * (beams - 1) + (1 if one_way else 2) * beams
    early += beams * (2 if one_way and ways == 1 else 3 * ways)
    late = (cols_count - 1) * (2 + beams) + (ways + 2) * beams + 3 * (beams - 1) + 3 * rows_count - 1
    vmem = pltpu.VMEM
    hbm = pl.BlockSpec(memory_space=pltpu.HBM)
    step, probe_gradient, loss = pl.pallas_call(
        functools.partial(whole_kernel, sizes, half, entries, positions),
        out_shape=[jax.ShapeDtypeStruct(s, f32) for s in (grid, pieces, (8, cols))],
        in_specs=[hbm] * 8,
        out_specs=vmem_specs(3),
        scratch_shapes=[
            pltpu.SMEM((count,), jnp.int32),
            pltpu.SMEM((count,), jnp.int32),
            vmem((beams, 2, depth, share, cols), phase_volume.dtype),
            vmem((beams, 2, share, cols), f32),
            vmem((beams - 1, 2, share, cols), f32),
            vmem((2, 3, tall, cols), f32),
            vmem(probe.shape, f32),
            vmem((count, length, length), amplitudes.dtype),
            vmem(left.shape, bf16),
            vmem(right.shape, bf16),
            vmem((4, 2, length, length), f32),
            vmem((4, 2 * length, length), bf16),
            vmem((4, length, 2 * length), bf16),
            vmem((4, 2 * length, length), bf16),
            vmem((4, length, 2 * length), bf16),
            vmem((4, 2, 3, 3 * length, cols), f32),
            vmem((2, 3, blocks, beams, thin, cols), f32),
            vmem((2 * length, length), f32),
            vmem((8, length), f32),
            vmem((2, 2, blocks, beams, thin, cols), f32),
            vmem((2, blocks, beams, thin, cols), f32),
            vmem((2, 2, beams, thin, cols), f32),
            vmem((beams, 2, blocks - 2, thin, cols), f32),
            vmem((beams - 1, 2, blocks - 2, thin, cols), f32),
            vmem(grid, f32),
            vmem((cols_count - 1, chunk, length), f32),
            vmem((beams,) + pieces[2:], f32),
            vmem((rows_count, beams - 1) + pieces[3:], f32),
            vmem(pieces[2:], f32),
            vmem((rows_count - 1,) + pieces[3:], f32),
            vmem((2, cols), f32),
            vmem((beams * rows_count - 1, 2, cols), f32),
            vmem((cols_count, 2, cols), f32),
            pltpu.SemaphoreType.DMA((beams,)),
            pltpu.SemaphoreType.DMA((6,)),
            pltpu.SemaphoreType.DMA((max(early, late),)),
            pltpu.SemaphoreType.DMA((early + late,)),
        ],
        compiler_params=pltpu.CompilerParams(
            collective_id=1, has_side_effects=True, vmem_limit_bytes=48 * 2**20
        ),
    )(
        pin(scan_rows.reshape(count)), pin(scan_cols.reshape(count)), pin(phase_volume), pin(absorb_volume), pin(probe),
        pin(amplitudes.reshape(count, length, length)), pin(left), pin(right),
    )
    step, probe_gradient, loss = pl.pallas_call(
        close_kernel,
        out_shape=[jax.ShapeDtypeStruct(s, f32) for s in (grid, pieces, (1, 1))],
        in_specs=vmem_specs(3),
        out_specs=[hbm] * 3,
        scratch_shapes=[vmem((1, 1), f32), pltpu.SemaphoreType.DMA((3,))],
        compiler_params=pltpu.CompilerParams(vmem_limit_bytes=2**20),
    )(step, probe_gradient, loss)
    return step.reshape(2, rows, cols), probe_gradient.reshape(probe.shape), loss.reshape(())


def solution(mesh):
    in_specs = (
        P("beam", "row", "col"),
        P("beam", "row", "col"),
        P(),
        P("row", "col", "beam", None, None),
        P("row", "col", "beam"),
        P("row", "col", "beam"),
    )
    out_specs = (P(None, "row", "col"), P(), P())
    return jax.shard_map(local, mesh=mesh, in_specs=in_specs, out_specs=out_specs, check_vma=False)
```

```python
import functools
import math

import jax
import jax.numpy as jnp
import numpy as np
from jax import lax
from jax.experimental import pallas as pl
from jax.experimental.pallas import tpu as pltpu
from jax.sharding import PartitionSpec as P


def dft_matrices(length):
    indices = np.arange(length, dtype=np.int32)
    product = indices[:, None] * indices[None, :] % length
    angles = product.astype(np.float32) * np.float32(2.0 * math.pi / length)
    factor = np.float32(1.0 / math.sqrt(length))
    real = (np.cos(angles) * factor).astype(jnp.bfloat16)
    imag = (-np.sin(angles) * factor).astype(jnp.bfloat16)
    left = np.block([[real, -imag], [imag, real]])
    right = np.block([[real, imag], [-imag, real]])
    return jnp.asarray(left), jnp.asarray(right)


def partners(me, count):
    if count == 4:
        flips = ((1, 1), (0, 1), (1, 0))
        return [lax.rem(me // 2 + up, 2) * 2 + lax.rem(me % 2 + across, 2) for up, across in flips]
    return [lax.rem(me + d, count) for d in range(1, count)]


class Sends:
    def __init__(self, sizes, send_sem, recv_sem):
        self.axes = {axis: (lax.axis_index(axis), count) for axis, count in sizes}
        self.sends, self.recvs = send_sem, recv_sem
        self.used = self.base = 0
        self.started = []

    def greet(self):
        self.barrier = pltpu.get_barrier_semaphore()
        targets = [{axis: other} for axis in self.axes for other in self.others(axis)]
        for target in targets:
            pl.semaphore_signal(self.barrier, inc=1, device_id=target, device_id_type=pl.DeviceIdType.MESH)
        return lambda: pl.semaphore_wait(self.barrier, len(targets))

    def others(self, axis):
        return partners(*self.axes[axis])

    def take(self):
        self.used += 1
        return self.used - 1

    def copy(self, target, src, dst, index=None):
        index = self.take() if index is None else index
        return pltpu.make_async_remote_copy(
            src_ref=src, dst_ref=dst, send_sem=self.sends.at[index - self.base],
            recv_sem=self.recvs.at[index], device_id=target,
            device_id_type=pl.DeviceIdType.MESH,
        )

    def send(self, target, src, dst):
        one = self.copy(target, src, dst)
        one.start()
        self.started.append(one.wait_send)
        return one

    def joint(self, slots):
        index = self.take()
        self.started.append(pltpu.make_async_copy(slots, slots, self.sends.at[index - self.base]).wait)
        return index, pltpu.make_async_copy(slots, slots, self.recvs.at[index]).wait

    def group(self, targets, src, slots):
        index, wait = self.joint(slots)
        for k, target in enumerate(targets):
            self.copy(target, src, slots.at[k], index).start()
        return wait

    def sides(self, axis, down, up, to_before=True, to_after=True, one_way=False, index=None):
        me, count = self.axes[axis]
        both = jnp.logical_and
        sends_before, sends_after = both(me > 0, to_before), both(me < count - 1, to_after)
        gets_after, gets_before = both(me < count - 1, to_before), both(me > 0, to_after)
        index = self.take() if index is None else index
        before = self.copy({axis: lax.rem(me + count - 1, count)}, *down, index)
        after = self.copy({axis: lax.rem(me + 1, count)}, *up, index if one_way or count == 2 else self.take())
        pl.when(sends_before)(before.start)
        pl.when(sends_after)(after.start)

        def wait_send():
            pl.when(sends_before)(before.wait_send)
            pl.when(sends_after)(after.wait_send)

        def wait_recv():
            pl.when(gets_after)(before.wait_recv)
            pl.when(gets_before)(after.wait_recv)

        self.started.append(wait_send)
        return wait_recv

    def finish(self):
        for wait_send in self.started:
            wait_send()
        self.started = []
        self.base = self.used


def tree(values):
    if len(values) == 4:
        return (values[3] + values[1]) + (values[2] + values[0])
    return functools.reduce(lambda a, b: a + b, values)


def vmem_specs(count):
    return [pl.BlockSpec(memory_space=pltpu.VMEM)] * count


def project(net, half, phase_ref, absorb_ref, out_ref, volume, part, slots, load_sem):
    beam, beams = net.axes["beam"]
    row, rows_count = net.axes["row"]
    depth, rows, cols = phase_ref.shape
    share = rows // beams
    edge = half // share
    blocks = rows // share + 2 * edge
    one_way = 2 * edge <= beams
    peers = net.others("beam")
    order = peers + [beam]
    for i, peer in enumerate(order):
        here = pl.ds(pl.multiple_of(peer * share, share), share)
        for plane, ref in enumerate((phase_ref, absorb_ref)):
            pltpu.make_async_copy(ref.at[:, here, :], volume.at[i, plane], load_sem.at[i]).start()
    arrived = net.greet()
    yield
    joint, scatter_wait = net.joint(slots)
    for i, peer in enumerate(order):
        pltpu.make_async_copy(volume.at[i], volume.at[i], load_sem.at[i]).wait()
        for plane in range(2):
            total = volume[i, plane, 0].astype(jnp.float32)
            for d in range(1, depth):
                total += volume[i, plane, d].astype(jnp.float32)
            part[i, plane] = total
        if i == 0:
            arrived()
        if i < beams - 1:
            net.copy({"beam": peer}, part.at[i], slots.at[i], joint).start()
    yield
    total = part[beams - 1]
    scatter_wait()
    for i in range(beams - 1):
        total += slots[i]
    at = lambda side, block: out_ref.at[:, side, pl.ds(pl.multiple_of(block * share, share), share), :]
    damping = jnp.exp(-total[1])
    own = edge + beam
    here = pl.ds(pl.multiple_of(own * share, share), share)
    out_ref[0, 1, here, :] = damping * jnp.cos(total[0])
    out_ref[1, 1, here, :] = damping * jnp.sin(total[0])
    arrivals = []

    def across(block, when=True, index=None):
        arrivals.append(net.sides(
            "col", (at(1, block), at(2, block)), (at(1, block), at(0, block)), when, when, index=index
        ))

    def rim_blocks(share_at):
        return lax.rem(edge + beams + share_at, blocks), lax.rem(edge + share_at + blocks - beams, blocks)

    def rim_here(share_at):
        from_after = jnp.logical_and(row < rows_count - 1, share_at < edge)
        from_before = jnp.logical_and(row > 0, share_at >= beams - edge)
        return from_after, from_before

    def along():
        below, above = rim_blocks(beam)
        wait = net.sides(
            "row", (at(1, own), at(1, below)), (at(1, own), at(1, above)), beam < edge, beam >= beams - edge,
            one_way=one_way,
        )
        return wait, below, above

    def around(peer, share_at):
        waits = []
        index = net.take()
        for block, here, there in zip(rim_blocks(share_at), rim_here(share_at), rim_here(peer)):
            one = net.copy({"beam": peer}, at(1, block), at(1, block), index)
            pl.when(here)(one.start)
            net.started.append(functools.partial(pl.when(here), one.wait_send))
            waits.append(functools.partial(pl.when(there), one.wait_recv))
            index = index if one_way or waits[1:] else net.take()
        return lambda: [wait() for wait in waits]

    def spread(share_at, below, above):
        from_after, from_before = rim_here(share_at)
        index = net.used if one_way and net.axes["col"][1] == 2 else None
        across(below, from_after)
        across(above, from_before, index)

    wait_rim, below, above = along()
    gather = [net.send({"beam": peer}, at(1, own), at(1, own)) for peer in peers]
    across(own)
    wait_rim()
    rims = [around(peer, beam) for peer in peers]
    spread(beam, below, above)
    for peer, one in zip(peers, gather):
        one.wait_recv()
        across(edge + peer)
    for peer, wait in zip(peers, rims):
        wait()
        spread(peer, *rim_blocks(peer))
    for wait in arrivals:
        wait()
    net.finish()
    yield


def windows(
    outer, rows_ref, cols_ref, trans_ref, probe_ref, amplitude_ref, left_ref, right_ref,
    canvas_ref, term_ref, misfit_ref, kept, wave, half, chi, back, moved,
):
    count, length = amplitude_ref.shape[:2]
    lanes = trans_ref.shape[3]
    spans = trans_ref.shape[1]
    inner = length // lanes
    step = 32
    steps = length // step
    dot = functools.partial(jnp.dot, preferred_element_type=jnp.float32)
    lane = lax.broadcasted_iota(jnp.int32, (step, lanes), 1)
    places = moved.shape[0]

    def enter(w, slot, m):
        row_at, col_at = rows_ref[w], cols_ref[w]
        shift = lax.rem(lanes - col_at, lanes)
        keep = lane < lanes - col_at
        here = pl.ds(m * step, step)
        planes = []
        for part in range(2):
            turned = [
                pltpu.roll(trans_ref[part, k, pl.ds(row_at + m * step, step), :], shift, 1)
                for k in range(spans)
            ]
            planes.append([jnp.where(keep, turned[k], turned[k + 1]) for k in range(inner)])
        for k in range(inner):
            real, imag = planes[0][k], planes[1][k]
            at = pl.ds(k * lanes, lanes)
            probe_real, probe_imag = probe_ref[0, here, at], probe_ref[1, here, at]
            kept[slot, 0, here, at] = real
            kept[slot, 1, here, at] = imag
            wave[slot, pl.ds(m * step, step), at] = (probe_real * real - probe_imag * imag).astype(jnp.bfloat16)
            wave[slot, pl.ds(length + m * step, step), at] = (probe_real * imag + probe_imag * real).astype(jnp.bfloat16)

    def compare(w, slot, m, far):
        here = pl.ds(m, step)
        real, imag = far[:, :length], far[:, length:]
        amplitude = amplitude_ref[w, here, :].astype(jnp.float32)
        square = real * real + imag * imag
        inverse = lax.rsqrt(jnp.maximum(square, 1.2e-38))
        off = square * inverse - amplitude
        misfit_ref[...] += jnp.sum((off * off).reshape(step // 8, 8, length), axis=0)
        ratio = 1.0 - amplitude * jnp.minimum(inverse, 2.0)
        chi[slot, here, :] = (real * ratio).astype(jnp.bfloat16)
        chi[slot, pl.ds(length + m, step), :] = (imag * ratio).astype(jnp.bfloat16)

    def leave(w, slot, m, grad):
        col_at = cols_ref[w]
        here, low = pl.ds(m, step), pl.ds(length + m, step)
        first = lane >= col_at
        objects = [[], []]
        for k in range(inner):
            at = pl.ds(k * lanes, lanes)
            grad_real = grad[:, k * lanes : (k + 1) * lanes]
            grad_imag = grad[:, length + k * lanes : length + (k + 1) * lanes]
            real, imag = kept[slot, 0, here, at], kept[slot, 1, here, at]
            term_real = real * grad_real + imag * grad_imag
            term_imag = real * grad_imag - imag * grad_real
            if w == 0:
                term_ref[here, at] = term_real
                term_ref[low, at] = term_imag
            else:
                term_ref[here, at] += term_real
                term_ref[low, at] += term_imag
            probe_real, probe_imag = probe_ref[0, here, at], probe_ref[1, here, at]
            objects[0].append(pltpu.roll(probe_real * term_imag - probe_imag * term_real, col_at, 1))
            objects[1].append(pltpu.roll(probe_real * term_real + probe_imag * term_imag, col_at, 1))
        for part in range(2):
            turned = objects[part]
            for k in range(spans):
                before = turned[k - 1] if k > 0 else 0.0
                after = turned[k] if k < inner else 0.0
                moved[w % places, part, k, pl.ds(length + m, step), :] = jnp.where(first, after, before)

    def left(values, first, out, slot):
        for k in range(2):
            part = dot(first[pl.ds(k * length, length), :], values[slot])
            out[slot, :, k * length : (k + 1) * length] = part.astype(jnp.bfloat16)

    def halves(make, source, table, w, slot, cut):
        tall = length // cut
        for c in range(cut):
            out = dot(source[slot, c * tall : (c + 1) * tall], table[...])
            for m in range(tall // step):
                make(w, slot, c * tall + m * step, out[m * step : (m + 1) * step])

    def enters(w):
        if w < count:
            for m in range(steps):
                enter(w, w % slots, m)

    def forth(w):
        if w < count:
            left(wave, left_ref, half, w % slots)

    def judge(w):
        if w < count:
            halves(compare, half, right_ref, w, w % slots, 1)

    def backs(w):
        if w < count:
            left(chi, right_ref, back, w % slots)

    def leaves(w):
        if 0 <= w < count:
            halves(leave, back, left_ref, w, w % slots, 1)

    def place(pair, block, b, k):
        thin = canvas_ref.shape[4]
        start = length + (block * canvas_ref.shape[3] + b) * thin
        for part in range(2):
            total = None if pair == 0 else canvas_ref[part, k, block, b]
            for w in (2 * pair, 2 * pair + 1):
                piece = moved[w % places, part, k, pl.ds(start - rows_ref[w], thin), :]
                total = piece if total is None else total + piece
            canvas_ref[part, k, block, b] = total

    def settle(pair):
        if 0 <= pair < pairs - 1:
            for block in range(canvas_ref.shape[2]):
                for share in range(canvas_ref.shape[3]):
                    for k in (1, *outer):
                        place(pair, block, share, k)

    slots = kept.shape[0]
    pairs = count // 2
    enters(0)
    enters(1)
    forth(0)
    for w in range(count):
        enters(w + 2)
        judge(w)
        forth(w + 1)
        leaves(w - 1)
        backs(w)
        if w % 2 == 0:
            settle(w // 2 - 1)
    leaves(count - 1)
    return functools.partial(place, pairs - 1)


def combine(
    net, outer, place, entries, positions, canvas_ref, term_ref, misfit_ref,
    step_ref, probe_ref, loss_ref,
    side, strip, rims, folded, folded_in, grads,
    term_col, term_a, term_beam, term_b, term_row, small, small_in, small_all,
):
    beam, beams = net.axes["beam"]
    row, rows_count = net.axes["row"]
    col, cols_count = net.axes["col"]
    blocks = strip.shape[1]
    cols = strip.shape[4]
    thin = term_b.shape[1]
    lines = rows_count * thin
    beam_peers, row_peers, col_peers = (net.others(axis) for axis in ("beam", "row", "col"))
    order = beam_peers + [beam]
    row_order = row_peers[::2] + row_peers[1::2] + [row]
    wide = [{"beam": b, "row": r} for b in order for r in row_peers + [row]][:-1]
    rows_of = lambda c, b, n: pl.ds(pl.multiple_of((c * beams + b) * lines, lines), n * lines)

    term_copies = [
        net.send({"col": c}, term_ref.at[rows_of(c, 0, beams), :], term_col.at[k])
        for k, c in enumerate(col_peers)
    ]
    across = []
    for p in order:
        for block in range(blocks):
            for k in outer:
                place(block, p, k)
        across.append(net.sides(
            "col",
            (canvas_ref.at[:, 0, :, p], side.at[1, :, :, p]),
            (canvas_ref.at[:, 2, :, p], side.at[0, :, :, p]),
        ))
    for p in order:
        for block in range(blocks):
            place(block, p, 1)
    for one in term_copies:
        one.wait_recv()
    for i, p in enumerate(order):
        total = term_ref[rows_of(col, p, 1), :]
        for k in range(cols_count - 1):
            total += term_col[k, pl.ds(pl.multiple_of(p * lines, lines), lines), :]
        for r in range(rows_count):
            term_a[i, r] = total[r * thin : (r + 1) * thin]
    term_beams = []
    for r in row_order:
        index = net.take()
        slots = term_beam.at[r]
        for i, p in enumerate(beam_peers):
            net.copy({"beam": p}, term_a.at[i, r], slots.at[i], index).start()
        net.started.append(pltpu.make_async_copy(slots, slots, net.sends.at[index - net.base]).wait)
        term_beams.append(pltpu.make_async_copy(slots, slots, net.recvs.at[index]).wait)

    along = []
    for i, p in enumerate(order):
        across[i]()
        if cols_count == 2:
            strip[:, :, p] = canvas_ref[:, 1, :, p] + side[1 - col, :, :, p]
        else:
            strip[:, :, p] = canvas_ref[:, 1, :, p] + side[0, :, :, p] + side[1, :, :, p]
        along.append(net.sides(
            "row",
            (strip.at[:, 0, p], rims.at[1, :, p]),
            (strip.at[:, blocks - 1, p], rims.at[0, :, p]),
        ))
    grid_index, grid_wait = net.joint(folded_in)

    def fold(i, p):
        along[i]()
        folded[i] = strip[:, 1 : blocks - 1, p]
        folded[i, :, 0] += rims[0, :, p]
        folded[i, :, blocks - 3] += rims[1, :, p]
        if i < beams - 1:
            net.copy({"beam": p}, folded.at[i], folded_in.at[i], grid_index).start()

    row_index, row_wait = net.joint(term_row)

    def gather(k, r):
        term_beams[k]()
        total = term_a[beams - 1, r]
        for i in range(beams - 1):
            total += term_beam[r, i]
        term_b[r] = total
        if k < rows_count - 1:
            net.copy({"row": r}, term_b.at[r], term_row.at[k], row_index).start()

    for i, p in enumerate(order):
        fold(i, p)
        if i < rows_count:
            gather(i, row_order[i])
    for k in range(beams, rows_count):
        gather(k, row_order[k])

    total = term_b[row]
    row_wait()
    for k in range(rows_count - 1):
        total += term_row[k]
    probe_ref[col, beam, row] = total * (1.0 / positions)
    piece = lambda r: probe_ref.at[col, beam, r]
    term_rows = [net.send({"row": r}, piece(row), piece(row)) for r in row_peers]
    around = [net.take() for _ in beam_peers]

    def forward(r):
        for p, index in zip(beam_peers, around):
            net.copy({"beam": p}, piece(r), piece(r), index).start()

    forward(row)

    total = folded[beams - 1]
    grid_wait()
    for i in range(beams - 1):
        total += folded_in[i]
    grads[0, :, beam] = total[0]
    grads[1, :, beam] = -total[1]
    misfit_sum = misfit_ref[:, :cols]
    for k in range(1, misfit_ref.shape[1] // cols):
        misfit_sum += misfit_ref[:, k * cols : (k + 1) * cols]
    small[:1] = jnp.sum((total * total).reshape(-1, cols), axis=0, keepdims=True)
    small[1:] = jnp.sum(misfit_sum, axis=0, keepdims=True)
    small_wait = net.group(wide, small, small_in)
    mine = grads.at[:, :, beam]
    grid_copies = [net.send({"beam": p}, mine, mine) for p in beam_peers]

    for r, one in zip(row_peers, term_rows):
        one.wait_recv()
        forward(r)
    share = lambda p: probe_ref.at[col, p]
    for index in around:
        net.started.append(pltpu.make_async_copy(share(beam), share(beam), net.sends.at[index - net.base]).wait)
    col_copies = [net.send({"col": c}, share(beam), share(beam)) for c in col_peers]
    small_wait()
    sums = [small_in[k] for k in range(beams * rows_count - 1)] + [small[...]]
    small_all[col] = tree([tree(sums[b * rows_count : (b + 1) * rows_count]) for b in range(beams)])
    smalls = [net.send({"col": c}, small_all.at[col], small_all.at[col]) for c in col_peers]
    for p, index in zip(beam_peers, around):
        pltpu.make_async_copy(share(p), share(p), net.recvs.at[index]).wait()
        col_copies += [net.send({"col": c}, share(p), share(p)) for c in col_peers]
    for one in grid_copies + smalls:
        one.wait_recv()
    total = small_all[0]
    for k in range(1, cols_count):
        total += small_all[k]
    mean_square = jnp.sum(total[:1], keepdims=True) / entries
    factor = jnp.minimum(1.0, 0.5 / jnp.sqrt(mean_square + 1e-06))
    step_ref[...] = grads[...] * factor[None, None, None]
    loss = jnp.sum(total[1:], keepdims=True) * (1.0 / (positions * misfit_ref.shape[1] ** 2))
    loss_ref[...] = jnp.broadcast_to(loss, loss_ref.shape)
    for one in col_copies:
        one.wait_recv()
    net.finish()
    assert net.used == net.recvs.shape[0]


def whole_kernel(
    sizes, half_length, entries, positions,
    rows_in, cols_in, phase_ref, absorb_ref, probe_in, amplitude_in, left_in, right_in,
    step_ref, probe_out, loss_ref,
    rows_ref, cols_ref, volume, part, slots, trans, probe, amplitude, left, right,
    kept, wave, half, chi, back, moved, canvas, term, misfit,
    side, strip, rims, folded, folded_in, grads,
    term_col, term_a, term_beam, term_b, term_row, small, small_in, small_all,
    load_sem, early_sem, send_sem, recv_sem,
):
    net = Sends(sizes, send_sem, recv_sem)
    row, rows_count = net.axes["row"]
    col, cols_count = net.axes["col"]
    stages = project(net, half_length, phase_ref, absorb_ref, trans, volume, part, slots, load_sem)
    next(stages)
    early = [
        pltpu.make_async_copy(src, dst, early_sem.at[k])
        for k, (src, dst) in enumerate(
            (
                (rows_in, rows_ref), (cols_in, cols_ref), (probe_in, probe),
                (left_in, left), (amplitude_in, amplitude), (right_in, right),
            )
        )
    ]
    misfit[...] = jnp.zeros_like(misfit)

    def empty(where):
        trans[(0,) + where] = jnp.ones_like(trans[(0,) + where])
        trans[(1,) + where] = jnp.zeros_like(trans[(1,) + where])

    for k, at in ((0, 0), (1, cols_count - 1)):

        @pl.when(col == at)
        def _():
            side[k] = jnp.zeros(side.shape[1:], jnp.float32)
            empty((2 * k,))

    for k, at in ((0, 0), (1, rows_count - 1)):

        @pl.when(row == at)
        def _():
            rims[k] = jnp.zeros(rims.shape[1:], jnp.float32)
            begin = k * (trans.shape[2] - half_length)
            for j in range(3):
                empty((j, pl.ds(begin, half_length)))

    length = probe.shape[1]
    blank = jnp.zeros(moved.shape[1:3] + (length, moved.shape[4]), jnp.float32)
    for k in range(moved.shape[0]):
        moved[k, :, :, :length, :] = blank
        moved[k, :, :, 2 * length :, :] = blank
    next(stages)
    for one in early:
        one.start()
    next(stages)
    for one in early:
        one.wait()
    outer = (2 - 2 * col,) if cols_count == 2 else (0, 2)
    place = windows(
        outer, rows_ref, cols_ref, trans, probe, amplitude, left, right,
        canvas, term, misfit, kept, wave, half, chi, back, moved,
    )
    combine(
        net, outer, place, entries, positions, canvas, term, misfit, step_ref, probe_out, loss_ref,
        side, strip, rims, folded, folded_in, grads,
        term_col, term_a, term_beam, term_b, term_row, small, small_in, small_all,
    )


def close_kernel(step_in, probe_in, loss_in, step_ref, probe_ref, loss_ref, one, sems):
    copies = [
        pltpu.make_async_copy(src, dst, sems.at[k])
        for k, (src, dst) in enumerate(((probe_in, probe_ref), (step_in, step_ref), (one, loss_ref)))
    ]
    copies[0].start()
    copies[1].start()
    one[...] = loss_in[:1, :1]
    copies[2].start()
    for copy in copies:
        copy.wait()


def pin(x):
    return pltpu.with_memory_space_constraint(x, pltpu.HBM)


def local(phase_volume, absorb_volume, probe, amplitudes, scan_rows, scan_cols):
    length = probe.shape[1]
    half = length // 2
    count = scan_rows.shape[2]
    depth, rows, cols = phase_volume.shape
    sizes = tuple((axis, lax.axis_size(axis)) for axis in ("beam", "row", "col"))
    counts = dict(sizes)
    beams, rows_count, cols_count = counts["beam"], counts["row"], counts["col"]
    positions = count * beams * rows_count * cols_count
    assert half == cols and count % 2 == 0
    left, right = dft_matrices(length)
    f32, bf16 = jnp.float32, jnp.bfloat16
    share = rows // beams
    tall = rows + 2 * half
    blocks = tall // half
    thin = half // beams
    chunk = 2 * length // cols_count
    lines = chunk // beams
    pieces = (cols_count, beams, rows_count, lines // rows_count, length)
    grid = (2, blocks - 2, beams, thin, cols)
    entries = 2 * rows * cols * rows_count * cols_count
    ways = 1 if cols_count == 2 else 2
    one_way = 2 * half <= rows
    early = beams + (1 if one_way else 2) * beams
    early += beams * (2 if one_way and ways == 1 else 3 * ways)
    late = (cols_count - 1) * (2 + beams) + (ways + 2) * beams + 2 * beams + 2 * rows_count
    vmem = pltpu.VMEM
    hbm = pl.BlockSpec(memory_space=pltpu.HBM)
    step, probe_gradient, loss = pl.pallas_call(
        functools.partial(whole_kernel, sizes, half, entries, positions),
        out_shape=[jax.ShapeDtypeStruct(s, f32) for s in (grid, pieces, (8, cols))],
        in_specs=[hbm] * 8,
        out_specs=vmem_specs(3),
        scratch_shapes=[
            pltpu.SMEM((count,), jnp.int32),
            pltpu.SMEM((count,), jnp.int32),
            vmem((beams, 2, depth, share, cols), phase_volume.dtype),
            vmem((beams, 2, share, cols), f32),
            vmem((beams - 1, 2, share, cols), f32),
            vmem((2, 3, tall, cols), f32),
            vmem(probe.shape, f32),
            vmem((count, length, length), amplitudes.dtype),
            vmem(left.shape, bf16),
            vmem(right.shape, bf16),
            vmem((4, 2, length, length), f32),
            vmem((4, 2 * length, length), bf16),
            vmem((4, length, 2 * length), bf16),
            vmem((4, 2 * length, length), bf16),
            vmem((4, length, 2 * length), bf16),
            vmem((4, 2, 3, 3 * length, cols), f32),
            vmem((2, 3, blocks, beams, thin, cols), f32),
            vmem((2 * length, length), f32),
            vmem((8, length), f32),
            vmem((2, 2, blocks, beams, thin, cols), f32),
            vmem((2, blocks, beams, thin, cols), f32),
            vmem((2, 2, beams, thin, cols), f32),
            vmem((beams, 2, blocks - 2, thin, cols), f32),
            vmem((beams - 1, 2, blocks - 2, thin, cols), f32),
            vmem(grid, f32),
            vmem((cols_count - 1, chunk, length), f32),
            vmem((beams,) + pieces[2:], f32),
            vmem((rows_count, beams - 1) + pieces[3:], f32),
            vmem(pieces[2:], f32),
            vmem((rows_count - 1,) + pieces[3:], f32),
            vmem((2, cols), f32),
            vmem((beams * rows_count - 1, 2, cols), f32),
            vmem((cols_count, 2, cols), f32),
            pltpu.SemaphoreType.DMA((beams,)),
            pltpu.SemaphoreType.DMA((6,)),
            pltpu.SemaphoreType.DMA((max(early, late),)),
            pltpu.SemaphoreType.DMA((early + late,)),
        ],
        compiler_params=pltpu.CompilerParams(
            collective_id=1, has_side_effects=True, vmem_limit_bytes=48 * 2**20
        ),
    )(
        pin(scan_rows.reshape(count)), pin(scan_cols.reshape(count)), pin(phase_volume), pin(absorb_volume), pin(probe),
        pin(amplitudes.reshape(count, length, length)), pin(left), pin(right),
    )
    step, probe_gradient, loss = pl.pallas_call(
        close_kernel,
        out_shape=[jax.ShapeDtypeStruct(s, f32) for s in (grid, pieces, (1, 1))],
        in_specs=vmem_specs(3),
        out_specs=[hbm] * 3,
        scratch_shapes=[vmem((1, 1), f32), pltpu.SemaphoreType.DMA((3,))],
        compiler_params=pltpu.CompilerParams(vmem_limit_bytes=2**20),
    )(step, probe_gradient, loss)
    return step.reshape(2, rows, cols), probe_gradient.reshape(probe.shape), loss.reshape(())


def solution(mesh):
    in_specs = (
        P("beam", "row", "col"),
        P("beam", "row", "col"),
        P(),
        P("row", "col", "beam", None, None),
        P("row", "col", "beam"),
        P("row", "col", "beam"),
    )
    out_specs = (P(None, "row", "col"), P(), P())
    return jax.shard_map(local, mesh=mesh, in_specs=in_specs, out_specs=out_specs, check_vma=False)
```
